32 devices in a mesh: dap: 32 (over z, y, x, core).
Axes of the slice: x: 2, y: 2, z: 4, core: 2. Of those that a mesh axis runs over, the one named last changes fastest.
Arguments:
- pair: bfloat16 [128, 128, 128], P('dap'), may hold values from -6 to 6
- residue_mask: int32 [128], P('dap'), may hold values 0 or 1
- norm_gain: float32 [2, 128], replicated, may hold values from 0.5 to 1.5
- proj_weight: bfloat16 [2, 128, 512], replicated, may hold values from -0.5 to 0.5
- gate_weight: bfloat16 [2, 128, 128], replicated, may hold values from -0.5 to 0.5
- mix_gain: float32 [2, 128], replicated, may hold values from 0.5 to 1.5
- out_weight: bfloat16 [2, 128, 128], replicated, may hold values from -0.5 to 0.5
Outputs:
- updated_pair: bfloat16 [128, 128, 128], P('dap')
The draws below stay inside these ranges and needn't reach their ends.
All inputs are finite; a program needn't handle non-finite values. No bound on the sum of `residue_mask` on one device may be relied on, other than what follows from the above.
Results may differ from the reference program's by a relative error of at most 0.0061.
Values may be sent and summed in bfloat16 or wider, within the bound.
A program may use at most 64 MiB of HBM per device.

```python
import jax
import jax.numpy as jnp
from jax import lax

C = 128
H = 128
ROWS = 4
N = 128
N_DAP = 32


def place_ends(result, own_key, smallest, largest):
    extent = result.shape
    spot = [jax.random.randint(jax.random.fold_in(own_key, axis), (), 0, extent[axis]) for axis in range(len(extent))]
    result = result.at[tuple(spot)].set(smallest)
    longest = extent.index(max(extent))
    spot[longest] = (spot[longest] + 1) % extent[longest]
    return result.at[tuple(spot)].set(largest)


def shard_levels(own_key, dims, pieces, smallest, high):
    level = 1.0
    for axis_at, blocks in pieces:
        heights = jax.random.uniform(jax.random.fold_in(jax.random.fold_in(own_key, 6), axis_at), (blocks,), jnp.float32, smallest / len(pieces), high / len(pieces))
        level = level * jnp.repeat(jnp.exp(heights), dims[axis_at] // blocks).reshape((-1,) + (1,) * (len(dims) - 1 - axis_at))
    return level


def noise(stream_key, dims, scale, bound, pieces=(), dtype=jnp.bfloat16):
    result = jax.random.normal(stream_key, dims, jnp.float32) * scale
    if len(pieces) > 0:
        result = shard_levels(stream_key, dims, pieces, -0.22, 0.18) * result
    return jnp.clip(result, min=-bound, max=bound).astype(dtype)


def setup_inputs(seed: int = 0) -> dict:
    key_list = jax.random.split(jax.random.key(seed), 8)
    return {
        "pair": noise(key_list[0], (N, N, C), 1.0, 6.0, ((0, 32),)),
        "residue_mask": place_ends((jax.random.randint(key_list[1], (N,), 0, 4) < 3).astype(jnp.int32), jax.random.fold_in(key_list[1], 1), 0, 1),
        "norm_gain": jnp.clip(jax.random.uniform(key_list[2], (2, C), jnp.float32, 0.5, 1.5), 0.5, 1.5),
        "proj_weight": noise(key_list[3], (2, C, 4 * H), C ** -0.5, 0.5),
        "gate_weight": noise(key_list[4], (2, C, C), C ** -0.5, 0.5),
        "mix_gain": jnp.clip(jax.random.uniform(key_list[5], (2, H), jnp.float32, 0.5, 1.5), 0.5, 1.5),
        "out_weight": noise(key_list[6], (2, H, C), H ** -0.5, 0.5),
    }


EPS = 1e-05

def normalize(values, axis):
    center = values - lax.optimization_barrier(jnp.mean(values, axis=axis, keepdims=True))
    spread = lax.optimization_barrier(jnp.mean(center * center, axis=axis, keepdims=True))
    return center * lax.rsqrt(spread + EPS)

def norm_rows(rows, gain):
    return (normalize(rows.astype(jnp.float32), 2) * gain).astype(jnp.bfloat16)

def panels(normed, mask_rows, mask_all, weight):
    proj = jnp.einsum('rnc,ch->hrn', normed.astype(jnp.float32), weight.astype(jnp.float32))
    hidden = weight.shape[1] // 4
    scale = mask_rows.astype(jnp.float32)[:, None] * mask_all.astype(jnp.float32)[None, :]
    left = (jax.nn.sigmoid(proj[:hidden]) * proj[hidden:2 * hidden] * scale).astype(jnp.bfloat16)
    right = (jax.nn.sigmoid(proj[2 * hidden:3 * hidden]) * proj[3 * hidden:] * scale).astype(jnp.bfloat16)
    return (left, right)

def finish(rows, normed, tri_rows, gate_w, tri_gain, out_w):
    gate = jax.nn.sigmoid(jnp.einsum('rnc,cd->rnd', normed.astype(jnp.float32), gate_w.astype(jnp.float32)))
    tri_normed = (normalize(tri_rows.astype(jnp.float32), 0) * tri_gain[:, None, None]).astype(jnp.bfloat16)
    out = jnp.einsum('hrn,hc->rnc', tri_normed.astype(jnp.float32), out_w.astype(jnp.float32))
    return (rows.astype(jnp.float32) + gate * out).astype(jnp.bfloat16)

def reference(pair, residue_mask, norm_gain, proj_weight, gate_weight, mix_gain, out_weight):
    total = pair.shape[0]
    chans = pair.shape[2]
    hidden = proj_weight.shape[2] // 4
    mask_blocks = residue_mask.reshape(N_DAP, ROWS)
    z = pair
    for layer in range(2):
        blocks = z.reshape(N_DAP, ROWS, total, chans)

        def make(args):
            rows, mrows = args
            normed = norm_rows(rows, norm_gain[layer])
            return panels(normed, mrows, residue_mask, proj_weight[layer])
        left, right = lax.map(make, (blocks, mask_blocks))
        left = left.transpose(1, 0, 2, 3).reshape(hidden, total, total)
        right = right.transpose(1, 0, 2, 3).reshape(hidden, total, total)

        def channel(args):
            one, two = args
            one = one.astype(jnp.float32)
            two = two.astype(jnp.float32)
            if layer == 0:
                prod = jnp.dot(one, two.T)
            else:
                prod = jnp.dot(one.T, two)
            return prod.astype(jnp.bfloat16)
        tri = lax.map(channel, (left, right))
        tri_blocks = tri.reshape(hidden, N_DAP, ROWS, total).transpose(1, 0, 2, 3)

        def close(args):
            rows, tri_rows = args
            normed = norm_rows(rows, norm_gain[layer])
            return finish(rows, normed, tri_rows, gate_weight[layer], mix_gain[layer], out_weight[layer])
        z = lax.map(close, (blocks, tri_blocks)).reshape(total, total, chans)
    return z
```

```python
import functools

import jax
import jax.numpy as jnp
from jax import lax
from jax.experimental import pallas as pl
from jax.experimental.pallas import tpu as pltpu
from jax.sharding import PartitionSpec as P

EPS = 1e-05
F32 = jnp.float32
BF16 = jnp.bfloat16
MESH = pl.DeviceIdType.MESH
HALVES = 2


def normalize(values, axis):
    center = values - jnp.mean(values, axis=axis, keepdims=True)
    spread = jnp.mean(center * center, axis=axis, keepdims=True)
    return center * lax.rsqrt(spread + EPS)


def dot(a, b, dims):
    return lax.dot_general(a, b, ((dims[:1], dims[1:]), ((), ())), preferred_element_type=F32)


def fused_kernel(
    devices,
    pair_hbm,
    mask_hbm,
    norm_hbm,
    proj_hbm,
    gate_hbm,
    mix_hbm,
    outw_hbm,
    out_ref,
    pair_ref,
    mask_ref,
    norm_ref,
    proj_ref,
    gate_ref,
    mix_ref,
    outw_ref,
    wide_send,
    wide_recv,
    cross_recv,
    tri_send,
    tri_recv,
    part_send,
    part_recv,
    mask_send,
    mask_recv,
    weight_s,
    gate_s,
    gain_s,
    state_s,
    stage_s,
    left_s,
    right_s,
    flat_s,
    part_s,
    square_s,
    send_sems,
    recv_sems,
    load_sems,
):
    sources = (pair_hbm, proj_hbm, mask_hbm, norm_hbm, gate_hbm, mix_hbm, outw_hbm)
    places = (pair_ref, proj_ref, mask_ref, norm_ref, gate_ref, mix_ref, outw_ref)
    loads = [
        pltpu.make_async_copy(source, place, load_sems.at[slot])
        for slot, (source, place) in enumerate(zip(sources, places))
    ]
    for load in loads:
        load.start()
    rows, total, chans = pair_ref.shape
    hidden = mix_ref.shape[1]
    group = devices // HALVES
    own = hidden // group
    me = lax.axis_index("dap")
    first = (me // group) * group
    spot = lax.rem(me, group)

    barrier = pltpu.get_barrier_semaphore()

    def greet(step, carry):
        peer = lax.rem(me + step, devices)
        pl.semaphore_signal(barrier, inc=1, device_id=(peer,), device_id_type=MESH)
        return carry

    lax.fori_loop(1, devices, greet, 0)

    def peer_of(step, size):
        if size != devices and size & (size - 1) == 0:
            return me ^ (size - step)
        base = (me // size) * size
        return base + lax.rem(me - base + step, size)

    def send_all(src, dst, size, slot):
        def one(step, carry):
            peer = peer_of(step, size)
            pltpu.make_async_remote_copy(
                src_ref=src(peer),
                dst_ref=dst,
                send_sem=send_sems.at[slot],
                recv_sem=recv_sems.at[slot],
                device_id=(peer,),
                device_id_type=MESH,
            ).start()
            return carry

        lax.fori_loop(1, size, one, 0)

    def wait_bytes(buf, count, sem):
        part = buf.at[pl.ds(0, count)]
        pltpu.make_async_copy(part, part, sem).wait()

    def turn_weights(layer):
        size = 4 * hidden
        i = lax.broadcasted_iota(jnp.int32, (size, size), 0)
        j = lax.broadcasted_iota(jnp.int32, (size, size), 1)
        pick = jnp.where(i == j, 1.0, 0.0).astype(BF16)
        weight_s[layer] = dot(pick, proj_ref[layer], (1, 1)).astype(BF16)

    def norm_of(layer):
        z = state_s[...].astype(F32)
        return (normalize(z, 1) * norm_ref[pl.ds(layer, 1), :]).astype(BF16)

    def make_panels(layer, normed, column_mask):
        for r in range(rows):
            scale = mask_ref[r].astype(F32)
            if column_mask is not None:
                scale = column_mask * scale
            part = normed[r * total : (r + 1) * total]
            for side in range(2):
                at = 2 * side * hidden
                gate = dot(weight_s[layer, at : at + hidden], part, (1, 1))
                value = dot(weight_s[layer, at + hidden : at + 2 * hidden], part, (1, 1))
                panel = jax.nn.sigmoid(gate) * value * scale
                wide_send[layer, side, :, r] = panel.reshape(group, own, total).astype(BF16)

    def make_gate(layer, normed):
        gate_s[...] = jax.nn.sigmoid(dot(normed, gate_ref[layer], (1, 0)))

    def unpack(panel, stage):
        for r in range(rows):
            stage[r] = panel[:, r].astype(F32).reshape(panel.shape[0] * own, total)

    def panel_of(stage, count, c):
        return [stage.at[r][pl.ds(c, count, stride=own), :] for r in range(rows)]

    def outgoing(mask_row):
        for c in range(own):
            for r, right in enumerate(panel_of(stage_s, devices, c)):
                square_s[c % 2, pl.ds(r, devices, stride=rows), :] = right
            left = jnp.concatenate(panel_of(left_s, group, c), axis=0)
            tri = dot((left * mask_row).astype(BF16), square_s[c % 2].astype(BF16), (1, 1))
            for r in range(rows):
                flat_s[pl.ds(c * rows + r, group, stride=own * rows), :] = tri[
                    r * group : (r + 1) * group
                ]
        tri_send[...] = flat_s[...].reshape(group, own * rows, total).astype(BF16)

    def incoming():
        for c in range(own):
            left = jnp.concatenate(panel_of(left_s, group, c), axis=0).astype(BF16)
            right = jnp.concatenate(panel_of(right_s, group, c), axis=0).astype(BF16)
            square_s[c % 2] = dot(left, right, (0, 0))
            for r in range(rows):
                part_s[pl.ds(c * rows + r, devices, stride=own * rows), :] = square_s[
                    c % 2, pl.ds(r, devices, stride=rows), :
                ]
        part_send[...] = part_s[...].reshape(devices, own * rows, total).astype(BF16)

    def finish(layer, products):
        flat_s[...] = products.reshape(hidden * rows, total)
        for r in range(rows):
            tri = flat_s[pl.ds(r, hidden, stride=rows), :]
            tri_normed = (normalize(tri, 0) * gain_s[layer]).astype(BF16)
            out = dot(tri_normed, outw_ref[layer], (0, 0))
            block = pl.ds(r * total, total)
            new = (state_s[block, :].astype(F32) + gate_s[block, :] * out).astype(BF16)
            if layer == 0:
                state_s[block, :] = new
            else:
                out_ref[r] = new

    for load in loads:
        load.wait()
    lane = lax.broadcasted_iota(jnp.int32, (1, total), 1)
    mask_row = jnp.zeros((1, total), F32)
    for r in range(rows):
        mask_row = mask_row + jnp.where(lane == me * rows + r, mask_ref[r].astype(F32), 0.0)
    mask_send[...] = mask_row
    state_s[...] = pair_ref[...].reshape(rows * total, chans)
    turn_weights(0)
    for layer in range(2):
        gain_s[layer] = jnp.broadcast_to(mix_ref[pl.ds(layer, 1), :], (total, hidden)).T
    normed = norm_of(0)
    make_panels(0, normed, None)
    pl.semaphore_wait(barrier, devices - 1)
    send_all(lambda peer: mask_send, mask_recv.at[me], devices, 0)
    send_all(
        lambda peer: wide_send.at[0, 1, lax.rem(peer, group)], cross_recv.at[me], devices, 1
    )
    send_all(
        lambda peer: wide_send.at[0, 0, lax.rem(peer, group)], wide_recv.at[0, spot], group, 2
    )
    mask_recv[me] = mask_send[...]
    cross_recv[me] = wide_send[0, 1, spot]
    wide_recv[0, spot] = wide_send[0, 0, spot]
    make_gate(0, normed)
    turn_weights(1)
    wait_bytes(mask_recv, devices - 1, recv_sems.at[0])
    column_mask = jnp.sum(mask_recv[...], axis=0)
    wait_bytes(wide_recv.at[0], group - 1, recv_sems.at[2])
    unpack(wide_recv[0], left_s)
    wait_bytes(cross_recv, devices - 1, recv_sems.at[1])
    unpack(cross_recv[...], stage_s)
    outgoing(column_mask)
    send_all(lambda peer: tri_send.at[peer - first], tri_recv.at[spot], group, 3)
    tri_recv[spot] = tri_send[spot]
    wait_bytes(tri_recv, group - 1, recv_sems.at[3])
    finish(0, tri_recv[...].astype(F32))
    normed = norm_of(1)
    make_panels(1, normed, column_mask)
    for side in range(2):
        send_all(
            lambda peer: wide_send.at[1, side, peer - first],
            wide_recv.at[1 + side, spot],
            group,
            4 + side,
        )
        wide_recv[1 + side, spot] = wide_send[1, side, spot]
    make_gate(1, normed)
    wait_bytes(wide_recv.at[1], group - 1, recv_sems.at[4])
    unpack(wide_recv[1], left_s)
    wait_bytes(wide_recv.at[2], group - 1, recv_sems.at[5])
    unpack(wide_recv[2], right_s)
    incoming()
    send_all(lambda peer: part_send.at[peer], part_recv.at[me], devices, 6)
    part_recv[me] = part_send[me]
    wait_bytes(mask_recv, devices - 1, send_sems.at[0])
    wait_bytes(cross_recv, devices - 1, send_sems.at[1])
    wait_bytes(wide_send.at[0, 0], group - 1, send_sems.at[2])
    wait_bytes(tri_send, group - 1, send_sems.at[3])
    wait_bytes(wide_send.at[1, 0], group - 1, send_sems.at[4])
    wait_bytes(wide_send.at[1, 1], group - 1, send_sems.at[5])
    wait_bytes(part_recv, devices - 1, recv_sems.at[6])
    products = part_recv[0:group].astype(F32)
    for half in range(1, HALVES):
        products = products + part_recv[half * group : (half + 1) * group].astype(F32)
    finish(1, products)
    wait_bytes(part_send, devices - 1, send_sems.at[6])


def fused(devices, pair, residue_mask, norm_gain, proj_weight, gate_weight, mix_gain, out_weight):
    rows, total, chans = pair.shape
    hidden = mix_gain.shape[1]
    group = devices // HALVES
    own = hidden // group
    hbm = pl.BlockSpec(memory_space=pltpu.HBM)
    params = (norm_gain, proj_weight, gate_weight, mix_gain, out_weight)
    return pl.pallas_call(
        functools.partial(fused_kernel, devices),
        out_shape=pltpu.VMEM((rows, total, chans), BF16),
        in_specs=[hbm] * 7,
        out_specs=pl.BlockSpec(memory_space=pltpu.VMEM),
        scratch_shapes=[
            pltpu.VMEM(pair.shape, BF16),
            pltpu.SMEM(residue_mask.shape, jnp.int32),
            *(pltpu.VMEM(p.shape, p.dtype) for p in params),
            pltpu.VMEM((2, 2, group, rows, own, total), BF16),
            pltpu.VMEM((3, group, rows, own, total), BF16),
            pltpu.VMEM((devices, rows, own, total), BF16),
            pltpu.VMEM((group, own * rows, total), BF16),
            pltpu.VMEM((group, own * rows, total), BF16),
            pltpu.VMEM((devices, own * rows, total), BF16),
            pltpu.VMEM((devices, own * rows, total), BF16),
            pltpu.VMEM((1, total), F32),
            pltpu.VMEM((devices, 1, total), F32),
            pltpu.VMEM((2, 4 * hidden, chans), BF16),
            pltpu.VMEM((rows * total, chans), F32),
            pltpu.VMEM((2, hidden, total), F32),
            pltpu.VMEM((rows * total, chans), BF16),
            pltpu.VMEM((rows, devices * own, total), F32),
            pltpu.VMEM((rows, group * own, total), F32),
            pltpu.VMEM((rows, group * own, total), F32),
            pltpu.VMEM((hidden * rows, total), F32),
            pltpu.VMEM((devices * own * rows, total), F32),
            pltpu.VMEM((2, total, total), F32),
            pltpu.SemaphoreType.DMA((7,)),
            pltpu.SemaphoreType.DMA((7,)),
            pltpu.SemaphoreType.DMA((7,)),
        ],
        compiler_params=pltpu.CompilerParams(
            collective_id=0, has_side_effects=True, vmem_limit_bytes=16777216
        ),
        name="triangles",
    )(*(pltpu.with_memory_space_constraint(v, pltpu.HBM) for v in (pair, residue_mask, *params)))


def panels(rows, mask_rows, mask_all, gain, weight):
    hidden = weight.shape[1] // 4
    mask_float = mask_all.astype(F32)
    normed = (normalize(rows.astype(F32), 2) * gain).astype(BF16)
    proj = jnp.einsum("rnc,ch->hrn", normed, weight, preferred_element_type=F32)
    scale = mask_rows.astype(F32)[:, None] * mask_float[None, :]
    left = (jax.nn.sigmoid(proj[:hidden]) * proj[hidden : 2 * hidden] * scale).astype(BF16)
    right = (jax.nn.sigmoid(proj[2 * hidden : 3 * hidden]) * proj[3 * hidden :] * scale).astype(
        BF16
    )
    return (normed, left, right)


def triangle(rows, mask_rows, mask_all, gain, weight, gate_w, tri_gain, out_w, second):
    normed, left, right = panels(rows, mask_rows, mask_all, gain, weight)
    left = lax.all_to_all(left, "dap", split_axis=0, concat_axis=1, tiled=True)
    right = lax.all_to_all(right, "dap", split_axis=0, concat_axis=1, tiled=True)
    spec = "cki,ckj->cij" if second else "cik,cjk->cij"
    tri = jnp.einsum(spec, left, right, preferred_element_type=F32).astype(BF16)
    tri = lax.all_to_all(tri, "dap", split_axis=1, concat_axis=0, tiled=True)
    gate = jax.nn.sigmoid(jnp.einsum("rnc,cd->rnd", normed, gate_w, preferred_element_type=F32))
    tri_normed = (normalize(tri.astype(F32), 0) * tri_gain[:, None, None]).astype(BF16)
    out = jnp.einsum("hrn,hc->rnc", tri_normed, out_w, preferred_element_type=F32)
    return (rows.astype(F32) + gate * out).astype(BF16)


def by_collectives(pair, residue_mask, *params):
    mask_all = lax.all_gather(residue_mask, "dap", axis=0, tiled=True)
    state = pair
    for layer in range(2):
        gain, weight, gate_w, tri_gain, out_w = (p[layer] for p in params)
        state = triangle(
            state, residue_mask, mask_all, gain, weight, gate_w, tri_gain, out_w, layer == 1
        )
    return state


def solution(mesh):
    devices = mesh.shape["dap"]

    def body(pair, residue_mask, norm_gain, proj_weight, gate_weight, mix_gain, out_weight):
        args = (pair, residue_mask, norm_gain, proj_weight, gate_weight, mix_gain, out_weight)
        group = devices // HALVES
        own = mix_gain.shape[1] // group
        whole = group * HALVES == devices and own * group == mix_gain.shape[1]
        if whole and own % 8 == 0 and pair.shape[1] == 128:
            return fused(devices, *args)
        return by_collectives(*args)

    return jax.shard_map(
        body,
        mesh=mesh,
        in_specs=(P("dap", None, None), P("dap"), P(), P(), P(), P(), P()),
        out_specs=P("dap", None, None),
        check_vma=False,
    )
```

```python
import contextlib
import functools

import jax
import jax.numpy as jnp
from jax import lax
from jax.experimental import pallas as pl
from jax.experimental.pallas import tpu as pltpu
from jax.sharding import PartitionSpec as P

EPS = 1e-05
F32 = jnp.float32
BF16 = jnp.bfloat16
MESH = pl.DeviceIdType.MESH
HALVES = 2


def normalize(values, axis):
    center = values - jnp.mean(values, axis=axis, keepdims=True)
    spread = jnp.mean(center * center, axis=axis, keepdims=True)
    return center * lax.rsqrt(spread + EPS)


def dot(a, b, dims):
    return lax.dot_general(a, b, ((dims[:1], dims[1:]), ((), ())), preferred_element_type=F32)


def mark(name):
    return contextlib.nullcontext()


def fused_kernel(
    devices,
    pair_hbm,
    mask_hbm,
    norm_hbm,
    proj_hbm,
    gate_hbm,
    mix_hbm,
    outw_hbm,
    out_ref,
    pair_ref,
    mask_ref,
    norm_ref,
    proj_ref,
    gate_ref,
    mix_ref,
    outw_ref,
    mask_send,
    mask_recv,
    a_send,
    a_near,
    a_far,
    pair_far,
    b_send,
    b_recv,
    c_send,
    c_near,
    c_far,
    back_recv,
    d_send,
    d_recv,
    weight_s,
    gatew_s,
    outw_s,
    mixg_s,
    normg_s,
    scale_s,
    normed_s,
    normed1_s,
    zt_s,
    z1t_s,
    gate0_s,
    z1_s,
    gate1_s,
    left_s,
    right_s,
    rhs_s,
    flat_s,
    lhs1_s,
    own1_s,
    far1_s,
    flat1_s,
    send_sems,
    recv_sems,
    load_sems,
):
    sources = (pair_hbm, proj_hbm, mask_hbm, norm_hbm, gate_hbm, mix_hbm, outw_hbm)
    places = (pair_ref, proj_ref, mask_ref, norm_ref, gate_ref, mix_ref, outw_ref)
    loads = [
        pltpu.make_async_copy(source, place, load_sems.at[slot])
        for slot, (source, place) in enumerate(zip(sources, places))
    ]
    for load in loads:
        load.start()
    rows, total, chans = pair_ref.shape
    hidden = mix_ref.shape[1]
    group = devices // HALVES
    own = hidden // group
    cols = total // HALVES
    spots = rows * cols
    pairs = rows // 2
    me = lax.axis_index("dap")
    half = me // group
    spot = lax.rem(me, group)
    partner = lax.rem(me + group, devices)
    near_cols = pl.ds(pl.multiple_of(half * cols, cols), cols)
    far_cols = pl.ds(pl.multiple_of((1 - half) * cols, cols), cols)

    barrier = pltpu.get_barrier_semaphore()

    def greet(step, carry):
        peer = me ^ (devices - step)
        pl.semaphore_signal(barrier, inc=1, device_id=(peer,), device_id_type=MESH)
        return carry

    lax.fori_loop(1, devices, greet, 0)

    def push(src, dst, slot, peer):
        pltpu.make_async_remote_copy(
            src_ref=src,
            dst_ref=dst,
            send_sem=send_sems.at[slot],
            recv_sem=recv_sems.at[slot],
            device_id=(peer,),
            device_id_type=MESH,
        ).start()

    def push_near(src, dst, slot):
        def one(step, carry):
            bits = group - step
            push(src(spot ^ bits), dst, slot, me ^ bits)
            return carry

        lax.fori_loop(1, group, one, 0)

    def push_far(src, dst, slot):
        def one(step, carry):
            bits = group - step
            push(src(spot ^ bits), dst, slot, me ^ (group + bits))
            return carry

        lax.fori_loop(1, group + 1, one, 0)

    def push_all(src, dst, slot):
        def one(step, carry):
            push(src, dst, slot, me ^ (devices - step))
            return carry

        lax.fori_loop(1, devices, one, 0)

    def wait_all(buf, sem):
        pltpu.make_async_copy(buf, buf, sem).wait()

    def wait_some(buf, count, sem):
        part = buf.at[pl.ds(0, count)]
        pltpu.make_async_copy(part, part, sem).wait()

    def lanes_of(parts):
        return jnp.concatenate(parts, axis=1)

    def panels_of(layer, normed, dims, side):
        at = 2 * side * hidden
        gate = dot(weight_s[layer, at : at + hidden], normed, dims)
        value = dot(weight_s[layer, at + hidden : at + 2 * hidden], normed, dims)
        return jax.nn.sigmoid(gate) * value

    def make_panels0():
        for pair in range(pairs):
            normed = normed_s[2 * pair : 2 * pair + 2].reshape(2 * total, chans)
            for side in range(2):
                panel = panels_of(0, normed, (1, 1), side)
                parts = [
                    (panel[:, r * total : (r + 1) * total] * mask_ref[2 * pair + r].astype(F32))
                    for r in range(2)
                ]
                tile = jnp.concatenate([p.reshape(group, own, total) for p in parts], axis=1)
                at = pl.ds(2 * own * pair, 2 * own)
                a_send[:, side, at, :] = tile.astype(BF16)

    def make_gate0(part, normed):
        gate0_s[part] = jax.nn.sigmoid(dot(gatew_s[...], normed, (1, 1)))

    def turn(values):
        return values.astype(F32).T.astype(BF16)

    def set_scale(part, owner, column_mask, doubled):
        entry = [
            jnp.sum(jnp.where(lane == owner * rows + r, column_mask, 0.0), axis=1, keepdims=True)
            for r in range(rows)
        ]
        scale_s[part] = lanes_of(
            [
                jnp.where(lane < cols, entry[2 * p], entry[2 * p + 1]) * doubled
                for p in range(pairs)
            ]
        )

    def outgoing(part, panel):
        left_s[part] = panel.astype(F32).reshape(group * rows * own, total)
        for c in range(own):
            left = jnp.concatenate(
                [
                    lanes_of(
                        [
                            left_s[part, pl.ds((2 * p + r) * own + c, group, stride=rows * own), :]
                            for r in range(2)
                        ]
                    )
                    for p in range(pairs)
                ],
                axis=0,
            ).astype(BF16)
            tri = dot(left, rhs_s[c], (1, 1))
            for p in range(pairs):
                flat_s[part, pl.ds(p * own + c, group, stride=pairs * own), :] = tri[
                    p * group : (p + 1) * group
                ]
        b_send[part] = flat_s[part].reshape(group, pairs * own, total).astype(BF16)

    def send_b(part):
        push_near(lambda at: b_send.at[part, at], b_recv.at[part, spot], 5 + part)
        b_recv[part, spot] = b_send[part, spot]

    def finish0(part):
        got = b_recv[part].astype(F32)
        tri = lanes_of(
            [got[:, p * own : (p + 1) * own].reshape(hidden, total) for p in range(pairs)]
        )
        gain = mixg_s[0]
        tri_normed = (normalize(tri, 0) * lanes_of([gain] * pairs)).astype(BF16)
        out = dot(outw_s[...], tri_normed, (1, 0))
        new = (zt_s[part].astype(F32) + gate0_s[part] * out).astype(BF16)
        z1t_s[part] = new
        normed = (normalize(new.astype(F32), 0) * lanes_of([normg_s[...]] * pairs)).astype(BF16)
        if part == 0:
            normed1_s[...] = normed
        for side in range(2):
            panel = panels_of(1, normed, (1, 0), side) * scale_s[part]
            tile = jnp.concatenate(
                [
                    panel[:, p * total : (p + 1) * total].reshape(group, own, total)
                    for p in range(pairs)
                ],
                axis=1,
            )
            c_send[part, :, side] = tile.astype(BF16)

    def send_c(part):
        push_far(lambda at: c_send.at[part, at, 1], c_far.at[part, spot], 9 + part)
        push_near(lambda at: c_send.at[part, at], c_near.at[part, spot], 7 + part)
        c_near[part, spot] = c_send[part, spot]

    def natural(part, normed):
        gate1_s[part] = jax.nn.sigmoid(dot(normed, gate_ref[1], (1, 0)))

    def unpack1(part):
        size = group * pairs * own
        at = pl.ds(part * size, size)
        near = c_near[part].astype(F32)
        lhs1_s[at, :] = near[:, 0].reshape(size, total)
        own1_s[at, :] = near[:, 1].reshape(size, total)
        far1_s[at, :] = c_far[1 - part].astype(F32).reshape(size, total)

    def incoming():
        count = HALVES * group * pairs
        low = lane < cols
        for c in range(own):
            pick = pl.ds(c, count, stride=own)
            left = lhs1_s[pick, :].astype(BF16)
            right = lanes_of([own1_s[pick, :], far1_s[pick, :]]).astype(BF16)
            prod = dot(left, right, (0, 0))
            straight = jnp.where(low, prod[:cols, :total], prod[cols:, total:])
            crossed = jnp.where(low, prod[:cols, total:], prod[cols:, :total])
            tri = straight + pltpu.roll(crossed, cols, 1)
            flat1_s[pl.ds(c, cols, stride=own), :] = tri
        d_send[...] = flat1_s[...].reshape(group, rows * own, total).astype(BF16)

    def finish1():
        got = d_recv[...].astype(F32)
        for r in range(rows):
            tri = got[:, r * own : (r + 1) * own].reshape(hidden, total)
            tri_normed = (normalize(tri, 0) * mixg_s[1]).astype(BF16)
            out = dot(tri_normed, outw_ref[1], (0, 0))
            block = pl.ds(r * cols, cols)
            for part, place in enumerate((near_cols, far_cols)):
                piece = out[part * cols : (part + 1) * cols]
                new = z1_s[part, block, :].astype(F32) + gate1_s[part, block, :] * piece
                out_ref[r, place, :] = new.astype(BF16)

    lane = lax.broadcasted_iota(jnp.int32, (1, total), 1)
    with mark("load"):
        for load in loads:
            load.wait()
    with mark("panels0"):
        mask_row = jnp.zeros((1, total), F32)
        for r in range(rows):
            mask_row = mask_row + jnp.where(lane == me * rows + r, mask_ref[r].astype(F32), 0.0)
        mask_send[...] = mask_row
        weight_s[0] = turn(proj_ref[0])
        z = pair_ref[...].reshape(rows * total, chans).astype(F32)
        normed = (normalize(z, 1) * norm_ref[pl.ds(0, 1), :]).astype(BF16)
        normed_s[...] = normed.reshape(rows, total, chans)
        make_panels0()
    with mark("barrier"):
        pl.semaphore_wait(barrier, devices - 1)
    with mark("sendA"):
        push_all(mask_send, mask_recv.at[me], 0)
        push_far(lambda at: a_send.at[at, 0], a_far.at[spot], 2)
        push_near(lambda at: a_send.at[at], a_near.at[spot], 1)
        push(pair_ref.at[:, far_cols, :], pair_far, 3, partner)
        mask_recv[me] = mask_send[...]
        a_near[spot] = a_send[spot]
    with mark("idleA"):
        gatew_s[...] = turn(gate_ref[0])
        outw_s[...] = turn(outw_ref[0])
        weight_s[1] = turn(proj_ref[1])
        for layer in range(2):
            mixg_s[layer] = jnp.broadcast_to(mix_ref[pl.ds(layer, 1), :], (total, hidden)).T
        normg_s[...] = jnp.broadcast_to(norm_ref[pl.ds(1, 1), :], (total, chans)).T
        rhs_s[...] = jnp.zeros(rhs_s.shape, BF16)
        zt_s[0] = turn(pair_ref[:, near_cols, :].reshape(spots, chans))
        make_gate0(0, normed_s[:, near_cols, :].reshape(spots, chans))
    with mark("waitmask"):
        wait_some(mask_recv, devices - 1, recv_sems.at[0])
    with mark("masks"):
        column_mask = jnp.sum(mask_recv[...], axis=0)
        doubled = jnp.where(lane // cols == half, column_mask, pltpu.roll(column_mask, cols, 1))
        set_scale(0, me, column_mask, doubled)
        set_scale(1, partner, column_mask, doubled)
    with mark("waitAnear"):
        wait_some(a_near, group - 1, recv_sems.at[1])
    with mark("out0"):
        right_s[...] = a_near[:, 1].astype(F32).reshape(group * rows * own, total)
        for c in range(own):
            right = (right_s[pl.ds(c, cols, stride=own), :] * column_mask).astype(BF16)
            rhs_s[c, 0:cols, 0:total] = right
            rhs_s[c, cols : 2 * cols, total : 2 * total] = right
        outgoing(0, a_near[:, 0])
    with mark("sendB0"):
        send_b(0)
    with mark("waitAfar"):
        wait_all(a_far, recv_sems.at[2])
    with mark("out1"):
        outgoing(1, a_far[...])
    with mark("sendB1"):
        send_b(1)
    with mark("waitB0"):
        wait_some(b_recv.at[0], group - 1, recv_sems.at[5])
    with mark("fin0"):
        finish0(0)
    with mark("sendC0"):
        send_c(0)
    with mark("waitpair"):
        wait_all(pair_far, recv_sems.at[3])
    with mark("pair"):
        z = pair_far[...].reshape(spots, chans)
        zt_s[1] = turn(z)
        make_gate0(1, (normalize(z.astype(F32), 1) * norm_ref[pl.ds(0, 1), :]).astype(BF16))
    with mark("waitB1"):
        wait_some(b_recv.at[1], group - 1, recv_sems.at[6])
    with mark("fin1"):
        finish0(1)
    with mark("sendC1"):
        send_c(1)
        push(z1t_s.at[1], back_recv, 4, partner)
    with mark("nat0"):
        z1_s[0] = z1t_s[0].astype(F32).T.astype(BF16)
        natural(0, normed1_s[...].astype(F32).T.astype(BF16))
    with mark("waitC0"):
        wait_some(c_near.at[0], group - 1, recv_sems.at[7])
        wait_all(c_far.at[0], recv_sems.at[9])
    with mark("waitC1"):
        wait_some(c_near.at[1], group - 1, recv_sems.at[8])
        wait_all(c_far.at[1], recv_sems.at[10])
    with mark("in"):
        unpack1(0)
        unpack1(1)
        incoming()
    with mark("sendD"):
        push_near(lambda at: d_send.at[at], d_recv.at[spot], 11)
        d_recv[spot] = d_send[spot]
    with mark("waitback"):
        wait_all(back_recv, recv_sems.at[4])
    with mark("nat1"):
        z = back_recv[...].astype(F32).T
        z1_s[1] = z.astype(BF16)
        natural(1, (normalize(z, 1) * norm_ref[pl.ds(1, 1), :]).astype(BF16))
        wait_some(mask_recv, devices - 1, send_sems.at[0])
        wait_some(a_near, group - 1, send_sems.at[1])
        wait_all(a_far, send_sems.at[2])
        wait_all(pair_far, send_sems.at[3])
        wait_all(back_recv, send_sems.at[4])
        for part in range(2):
            wait_some(b_recv.at[part], group - 1, send_sems.at[5 + part])
            wait_some(c_near.at[part], group - 1, send_sems.at[7 + part])
            wait_all(c_far.at[part], send_sems.at[9 + part])
    with mark("waitD"):
        wait_some(d_recv, group - 1, recv_sems.at[11])
    with mark("finish1"):
        finish1()
    wait_some(d_recv, group - 1, send_sems.at[11])


def fused(devices, pair, residue_mask, norm_gain, proj_weight, gate_weight, mix_gain, out_weight):
    rows, total, chans = pair.shape
    hidden = mix_gain.shape[1]
    group = devices // HALVES
    own = hidden // group
    cols = total // HALVES
    spots = rows * cols
    pairs = rows // 2
    half_rows = group * pairs * own
    hbm = pl.BlockSpec(memory_space=pltpu.HBM)
    params = (norm_gain, proj_weight, gate_weight, mix_gain, out_weight)
    operands = [
        pltpu.with_memory_space_constraint(v, pltpu.HBM) for v in (pair, residue_mask, *params)
    ]
    return pl.pallas_call(
        functools.partial(fused_kernel, devices),
        out_shape=pltpu.VMEM(pair.shape, BF16),
        in_specs=[hbm] * 7,
        out_specs=pl.BlockSpec(memory_space=pltpu.VMEM),
        scratch_shapes=[
            pltpu.VMEM(pair.shape, BF16),
            pltpu.SMEM(residue_mask.shape, jnp.int32),
            *(pltpu.VMEM(p.shape, p.dtype) for p in params),
            pltpu.VMEM((1, total), F32),
            pltpu.VMEM((devices, 1, total), F32),
            pltpu.VMEM((group, 2, rows * own, total), BF16),
            pltpu.VMEM((group, 2, rows * own, total), BF16),
            pltpu.VMEM((group, rows * own, total), BF16),
            pltpu.VMEM((rows, cols, chans), BF16),
            pltpu.VMEM((2, group, pairs * own, total), BF16),
            pltpu.VMEM((2, group, pairs * own, total), BF16),
            pltpu.VMEM((2, group, 2, pairs * own, total), BF16),
            pltpu.VMEM((2, group, 2, pairs * own, total), BF16),
            pltpu.VMEM((2, group, pairs * own, total), BF16),
            pltpu.VMEM((chans, spots), BF16),
            pltpu.VMEM((group, rows * own, total), BF16),
            pltpu.VMEM((group, rows * own, total), BF16),
            pltpu.VMEM((2, 4 * hidden, chans), BF16),
            pltpu.VMEM((chans, chans), BF16),
            pltpu.VMEM((chans, hidden), BF16),
            pltpu.VMEM((2, hidden, total), F32),
            pltpu.VMEM((chans, total), F32),
            pltpu.VMEM((2, 1, spots), F32),
            pltpu.VMEM((rows, total, chans), BF16),
            pltpu.VMEM((chans, spots), BF16),
            pltpu.VMEM((2, chans, spots), BF16),
            pltpu.VMEM((2, chans, spots), BF16),
            pltpu.VMEM((2, chans, spots), F32),
            pltpu.VMEM((2, spots, chans), BF16),
            pltpu.VMEM((2, spots, chans), F32),
            pltpu.VMEM((2, group * rows * own, total), F32),
            pltpu.VMEM((group * rows * own, total), F32),
            pltpu.VMEM((own, total, 2 * total), BF16),
            pltpu.VMEM((2, half_rows, total), F32),
            pltpu.VMEM((2 * half_rows, total), F32),
            pltpu.VMEM((2 * half_rows, total), F32),
            pltpu.VMEM((2 * half_rows, total), F32),
            pltpu.VMEM((cols * own, total), F32),
            pltpu.SemaphoreType.DMA((12,)),
            pltpu.SemaphoreType.DMA((12,)),
            pltpu.SemaphoreType.DMA((7,)),
        ],
        compiler_params=pltpu.CompilerParams(
            collective_id=0, has_side_effects=True, vmem_limit_bytes=16777216
        ),
        name="triangles",
    )(*operands)


def panels(rows, mask_rows, mask_all, gain, weight):
    hidden = weight.shape[1] // 4
    mask_float = mask_all.astype(F32)
    normed = (normalize(rows.astype(F32), 2) * gain).astype(BF16)
    proj = jnp.einsum("rnc,ch->hrn", normed, weight, preferred_element_type=F32)
    scale = mask_rows.astype(F32)[:, None] * mask_float[None, :]
    left = (jax.nn.sigmoid(proj[:hidden]) * proj[hidden : 2 * hidden] * scale).astype(BF16)
    right = (jax.nn.sigmoid(proj[2 * hidden : 3 * hidden]) * proj[3 * hidden :] * scale).astype(
        BF16
    )
    return (normed, left, right)


def triangle(rows, mask_rows, mask_all, gain, weight, gate_w, tri_gain, out_w, second):
    normed, left, right = panels(rows, mask_rows, mask_all, gain, weight)
    left = lax.all_to_all(left, "dap", split_axis=0, concat_axis=1, tiled=True)
    right = lax.all_to_all(right, "dap", split_axis=0, concat_axis=1, tiled=True)
    spec = "cki,ckj->cij" if second else "cik,cjk->cij"
    tri = jnp.einsum(spec, left, right, preferred_element_type=F32).astype(BF16)
    tri = lax.all_to_all(tri, "dap", split_axis=1, concat_axis=0, tiled=True)
    gate = jax.nn.sigmoid(jnp.einsum("rnc,cd->rnd", normed, gate_w, preferred_element_type=F32))
    tri_normed = (normalize(tri.astype(F32), 0) * tri_gain[:, None, None]).astype(BF16)
    out = jnp.einsum("hrn,hc->rnc", tri_normed, out_w, preferred_element_type=F32)
    return (rows.astype(F32) + gate * out).astype(BF16)


def by_collectives(pair, residue_mask, *params):
    mask_all = lax.all_gather(residue_mask, "dap", axis=0, tiled=True)
    state = pair
    for layer in range(2):
        gain, weight, gate_w, tri_gain, out_w = (p[layer] for p in params)
        state = triangle(
            state, residue_mask, mask_all, gain, weight, gate_w, tri_gain, out_w, layer == 1
        )
    return state


def solution(mesh):
    devices = mesh.shape["dap"]

    def body(pair, residue_mask, norm_gain, proj_weight, gate_weight, mix_gain, out_weight):
        args = (pair, residue_mask, norm_gain, proj_weight, gate_weight, mix_gain, out_weight)
        group = devices // HALVES
        own = mix_gain.shape[1] // group
        rows, total, chans = pair.shape
        whole = group * HALVES == devices and group & (group - 1) == 0
        whole = whole and own * group == chans == mix_gain.shape[1] == total == 128
        if whole and own == 8 and rows == 4:
            return fused(devices, *args)
        return by_collectives(*args)

    return jax.shard_map(
        body,
        mesh=mesh,
        in_specs=(P("dap", None, None), P("dap"), P(), P(), P(), P(), P()),
        out_specs=P("dap", None, None),
        check_vma=False,
    )
```

```python
import contextlib
import functools

import jax
import jax.numpy as jnp
from jax import lax
from jax.experimental import pallas as pl
from jax.experimental.pallas import tpu as pltpu
from jax.sharding import PartitionSpec as P

EPS = 1e-05
F32 = jnp.float32
BF16 = jnp.bfloat16
MESH = pl.DeviceIdType.MESH
HALVES = 2


def normalize(values, axis):
    center = values - jnp.mean(values, axis=axis, keepdims=True)
    spread = jnp.mean(center * center, axis=axis, keepdims=True)
    return center * lax.rsqrt(spread + EPS)


def dot(a, b, dims):
    return lax.dot_general(a, b, ((dims[:1], dims[1:]), ((), ())), preferred_element_type=F32)


def mark(name):
    return contextlib.nullcontext()


def fused_kernel(
    devices,
    pair_hbm,
    mask_hbm,
    norm_hbm,
    proj_hbm,
    gate_hbm,
    mix_hbm,
    outw_hbm,
    out_ref,
    pair_ref,
    mask_ref,
    norm_ref,
    proj_ref,
    gate_ref,
    mix_ref,
    outw_ref,
    mask_send,
    mask_recv,
    a_send,
    a_near,
    a_far,
    pair_far,
    b_send,
    b_recv,
    c_send,
    c_near,
    c_far,
    back_recv,
    d_send,
    d_recv,
    weight_s,
    gatew_s,
    outw_s,
    mixg_s,
    normg_s,
    scale_s,
    normed_s,
    normed1_s,
    zt_s,
    z1t_s,
    gate0_s,
    z1_s,
    gate1_s,
    left_s,
    right_s,
    rhs_s,
    flat_s,
    lhs1_s,
    own1_s,
    far1_s,
    flat1_s,
    send_sems,
    recv_sems,
    load_sems,
):
    sources = (pair_hbm, proj_hbm, mask_hbm, norm_hbm, gate_hbm, mix_hbm, outw_hbm)
    places = (pair_ref, proj_ref, mask_ref, norm_ref, gate_ref, mix_ref, outw_ref)
    loads = [
        pltpu.make_async_copy(source, place, load_sems.at[slot])
        for slot, (source, place) in enumerate(zip(sources, places))
    ]
    for load in loads:
        load.start()
    rows, total, chans = pair_ref.shape
    hidden = mix_ref.shape[1]
    group = devices // HALVES
    own = hidden // group
    cols = total // HALVES
    spots = rows * cols
    pairs = rows // 2
    me = lax.axis_index("dap")
    half = me // group
    spot = lax.rem(me, group)
    partner = lax.rem(me + group, devices)
    zone = me * 4 // devices
    flip = jnp.where((zone == 0) | (zone == 3), group // 2, 0)
    near_cols = pl.ds(pl.multiple_of(half * cols, cols), cols)
    far_cols = pl.ds(pl.multiple_of((1 - half) * cols, cols), cols)

    barrier = pltpu.get_barrier_semaphore()

    def greet(step, carry):
        peer = me ^ (devices - step)
        pl.semaphore_signal(barrier, inc=1, device_id=(peer,), device_id_type=MESH)
        return carry

    lax.fori_loop(1, devices, greet, 0)

    def push(src, dst, slot, peer):
        pltpu.make_async_remote_copy(
            src_ref=src,
            dst_ref=dst,
            send_sem=send_sems.at[slot],
            recv_sem=recv_sems.at[slot],
            device_id=(peer,),
            device_id_type=MESH,
        ).start()

    def push_near(src, dst, slot):
        def one(step, carry):
            bits = group - step
            push(src(spot ^ bits), dst, slot, me ^ bits)
            return carry

        lax.fori_loop(1, group, one, 0)

    def push_far(src, dst, slot):
        def one(step, carry):
            bits = (group - step) ^ flip
            push(src(spot ^ bits), dst, slot, me ^ (group + bits))
            return carry

        lax.fori_loop(1, group + 1, one, 0)

    def push_all(src, dst, slot):
        def one(step, carry):
            push(src, dst, slot, me ^ (devices - step))
            return carry

        lax.fori_loop(1, devices, one, 0)

    def wait_all(buf, sem):
        pltpu.make_async_copy(buf, buf, sem).wait()

    def wait_some(buf, count, sem):
        part = buf.at[pl.ds(0, count)]
        pltpu.make_async_copy(part, part, sem).wait()

    def lanes_of(parts):
        return jnp.concatenate(parts, axis=1)

    def panels_of(layer, normed, dims, side):
        at = 2 * side * hidden
        gate = dot(weight_s[layer, at : at + hidden], normed, dims)
        value = dot(weight_s[layer, at + hidden : at + 2 * hidden], normed, dims)
        return jax.nn.sigmoid(gate) * value

    def make_panels0():
        for pair in range(pairs):
            normed = normed_s[2 * pair : 2 * pair + 2].reshape(2 * total, chans)
            for side in range(2):
                panel = panels_of(0, normed, (1, 1), side)
                parts = [
                    (panel[:, r * total : (r + 1) * total] * mask_ref[2 * pair + r].astype(F32))
                    for r in range(2)
                ]
                tile = jnp.concatenate([p.reshape(group, own, total) for p in parts], axis=1)
                at = pl.ds(2 * own * pair, 2 * own)
                a_send[:, side, at, :] = tile.astype(BF16)

    def make_gate0(part, normed):
        gate0_s[part] = jax.nn.sigmoid(dot(gatew_s[...], normed, (1, 1)))

    def turn(values):
        return values.astype(F32).T.astype(BF16)

    def set_scale(part, owner, column_mask, doubled):
        entry = [
            jnp.sum(jnp.where(lane == owner * rows + r, column_mask, 0.0), axis=1, keepdims=True)
            for r in range(rows)
        ]
        scale_s[part] = lanes_of(
            [
                jnp.where(lane < cols, entry[2 * p], entry[2 * p + 1]) * doubled
                for p in range(pairs)
            ]
        )

    def outgoing(part, panel):
        left_s[part] = panel.astype(F32).reshape(group * rows * own, total)
        for c in range(own):
            left = jnp.concatenate(
                [
                    lanes_of(
                        [
                            left_s[part, pl.ds((2 * p + r) * own + c, group, stride=rows * own), :]
                            for r in range(2)
                        ]
                    )
                    for p in range(pairs)
                ],
                axis=0,
            ).astype(BF16)
            tri = dot(left, rhs_s[c], (1, 1))
            for p in range(pairs):
                flat_s[part, pl.ds(p * own + c, group, stride=pairs * own), :] = tri[
                    p * group : (p + 1) * group
                ]
        b_send[part] = flat_s[part].reshape(group, pairs * own, total).astype(BF16)

    def send_b(part):
        push_near(lambda at: b_send.at[part, at], b_recv.at[part, spot], 5 + part)
        b_recv[part, spot] = b_send[part, spot]

    def finish0(part):
        got = b_recv[part].astype(F32)
        tri = lanes_of(
            [got[:, p * own : (p + 1) * own].reshape(hidden, total) for p in range(pairs)]
        )
        gain = mixg_s[0]
        tri_normed = (normalize(tri, 0) * lanes_of([gain] * pairs)).astype(BF16)
        out = dot(outw_s[...], tri_normed, (1, 0))
        new = (zt_s[part].astype(F32) + gate0_s[part] * out).astype(BF16)
        z1t_s[part] = new
        normed = (normalize(new.astype(F32), 0) * lanes_of([normg_s[...]] * pairs)).astype(BF16)
        if part == 0:
            normed1_s[...] = normed
        for side in range(2):
            panel = panels_of(1, normed, (1, 0), side) * scale_s[part]
            tile = jnp.concatenate(
                [
                    panel[:, p * total : (p + 1) * total].reshape(group, own, total)
                    for p in range(pairs)
                ],
                axis=1,
            )
            c_send[part, :, side] = tile.astype(BF16)

    def send_c(part):
        push_far(lambda at: c_send.at[part, at, 1], c_far.at[part, spot], 9 + part)
        push_near(lambda at: c_send.at[part, at], c_near.at[part, spot], 7 + part)
        c_near[part, spot] = c_send[part, spot]

    def natural(part, normed):
        gate1_s[part] = jax.nn.sigmoid(dot(normed, gate_ref[1], (1, 0)))

    def unpack1(part):
        size = group * pairs * own
        at = pl.ds(part * size, size)
        near = c_near[part].astype(F32)
        lhs1_s[at, :] = near[:, 0].reshape(size, total)
        own1_s[at, :] = near[:, 1].reshape(size, total)
        far1_s[at, :] = c_far[1 - part].astype(F32).reshape(size, total)

    def incoming():
        count = HALVES * group * pairs
        low = lane < cols
        for c in range(own):
            pick = pl.ds(c, count, stride=own)
            left = lhs1_s[pick, :].astype(BF16)
            right = lanes_of([own1_s[pick, :], far1_s[pick, :]]).astype(BF16)
            prod = dot(left, right, (0, 0))
            straight = jnp.where(low, prod[:cols, :total], prod[cols:, total:])
            crossed = jnp.where(low, prod[:cols, total:], prod[cols:, :total])
            tri = straight + pltpu.roll(crossed, cols, 1)
            flat1_s[pl.ds(c, cols, stride=own), :] = tri
        d_send[...] = flat1_s[...].reshape(group, rows * own, total).astype(BF16)

    def finish1():
        got = d_recv[...].astype(F32)
        for r in range(rows):
            tri = got[:, r * own : (r + 1) * own].reshape(hidden, total)
            tri_normed = (normalize(tri, 0) * mixg_s[1]).astype(BF16)
            out = dot(tri_normed, outw_ref[1], (0, 0))
            block = pl.ds(r * cols, cols)
            for part, place in enumerate((near_cols, far_cols)):
                piece = out[part * cols : (part + 1) * cols]
                new = z1_s[part, block, :].astype(F32) + gate1_s[part, block, :] * piece
                out_ref[r, place, :] = new.astype(BF16)

    lane = lax.broadcasted_iota(jnp.int32, (1, total), 1)
    with mark("load"):
        for load in loads:
            load.wait()
    with mark("panels0"):
        mask_row = jnp.zeros((1, total), F32)
        for r in range(rows):
            mask_row = mask_row + jnp.where(lane == me * rows + r, mask_ref[r].astype(F32), 0.0)
        mask_send[...] = mask_row
        weight_s[0] = turn(proj_ref[0])
        z = pair_ref[...].reshape(rows * total, chans).astype(F32)
        normed = (normalize(z, 1) * norm_ref[pl.ds(0, 1), :]).astype(BF16)
        normed_s[...] = normed.reshape(rows, total, chans)
        make_panels0()
    with mark("barrier"):
        pl.semaphore_wait(barrier, devices - 1)
    with mark("sendA"):
        push_all(mask_send, mask_recv.at[me], 0)
        push_near(lambda at: a_send.at[at], a_near.at[spot], 1)
        push_far(lambda at: a_send.at[at, 0], a_far.at[spot], 2)
        mask_recv[me] = mask_send[...]
        a_near[spot] = a_send[spot]
    with mark("idleA"):
        gatew_s[...] = turn(gate_ref[0])
        outw_s[...] = turn(outw_ref[0])
        weight_s[1] = turn(proj_ref[1])
        for layer in range(2):
            mixg_s[layer] = jnp.broadcast_to(mix_ref[pl.ds(layer, 1), :], (total, hidden)).T
        normg_s[...] = jnp.broadcast_to(norm_ref[pl.ds(1, 1), :], (total, chans)).T
        rhs_s[...] = jnp.zeros(rhs_s.shape, BF16)
        zt_s[0] = turn(pair_ref[:, near_cols, :].reshape(spots, chans))
        make_gate0(0, normed_s[:, near_cols, :].reshape(spots, chans))
    with mark("waitmask"):
        wait_some(mask_recv, devices - 1, recv_sems.at[0])
    with mark("masks"):
        column_mask = jnp.sum(mask_recv[...], axis=0)
        doubled = jnp.where(lane // cols == half, column_mask, pltpu.roll(column_mask, cols, 1))
        set_scale(0, me, column_mask, doubled)
        set_scale(1, partner, column_mask, doubled)
    with mark("waitAnear"):
        wait_some(a_near, group - 1, recv_sems.at[1])
    with mark("out0"):
        right_s[...] = a_near[:, 1].astype(F32).reshape(group * rows * own, total)
        for c in range(own):
            right = (right_s[pl.ds(c, cols, stride=own), :] * column_mask).astype(BF16)
            rhs_s[c, 0:cols, 0:total] = right
            rhs_s[c, cols : 2 * cols, total : 2 * total] = right
        outgoing(0, a_near[:, 0])
    with mark("sendB0"):
        send_b(0)
        push(pair_ref.at[:, far_cols, :], pair_far, 3, partner)
    with mark("waitAfar"):
        wait_all(a_far, recv_sems.at[2])
    with mark("out1"):
        outgoing(1, a_far[...])
    with mark("sendB1"):
        send_b(1)
    with mark("waitB0"):
        wait_some(b_recv.at[0], group - 1, recv_sems.at[5])
    with mark("fin0"):
        finish0(0)
    with mark("sendC0"):
        send_c(0)
    with mark("waitpair"):
        wait_all(pair_far, recv_sems.at[3])
    with mark("pair"):
        z = pair_far[...].reshape(spots, chans)
        zt_s[1] = turn(z)
        make_gate0(1, (normalize(z.astype(F32), 1) * norm_ref[pl.ds(0, 1), :]).astype(BF16))
    with mark("waitB1"):
        wait_some(b_recv.at[1], group - 1, recv_sems.at[6])
    with mark("fin1"):
        finish0(1)
    with mark("sendC1"):
        send_c(1)
    with mark("nat0"):
        z1_s[0] = z1t_s[0].astype(F32).T.astype(BF16)
        natural(0, normed1_s[...].astype(F32).T.astype(BF16))
    with mark("back"):
        wait_all(c_far.at[1], send_sems.at[10])
        push(z1t_s.at[1], back_recv, 4, partner)
    with mark("waitC0"):
        wait_some(c_near.at[0], group - 1, recv_sems.at[7])
        wait_all(c_far.at[0], recv_sems.at[9])
    with mark("waitC1"):
        wait_some(c_near.at[1], group - 1, recv_sems.at[8])
        wait_all(c_far.at[1], recv_sems.at[10])
    with mark("in"):
        unpack1(0)
        unpack1(1)
        incoming()
    with mark("sendD"):
        push_near(lambda at: d_send.at[at], d_recv.at[spot], 11)
        d_recv[spot] = d_send[spot]
    with mark("waitback"):
        wait_all(back_recv, recv_sems.at[4])
    with mark("nat1"):
        z = back_recv[...].astype(F32).T
        z1_s[1] = z.astype(BF16)
        natural(1, (normalize(z, 1) * norm_ref[pl.ds(1, 1), :]).astype(BF16))
        wait_some(mask_recv, devices - 1, send_sems.at[0])
        wait_some(a_near, group - 1, send_sems.at[1])
        wait_all(a_far, send_sems.at[2])
        wait_all(pair_far, send_sems.at[3])
        wait_all(back_recv, send_sems.at[4])
        wait_all(c_far.at[0], send_sems.at[9])
        for part in range(2):
            wait_some(b_recv.at[part], group - 1, send_sems.at[5 + part])
            wait_some(c_near.at[part], group - 1, send_sems.at[7 + part])
    with mark("waitD"):
        wait_some(d_recv, group - 1, recv_sems.at[11])
    with mark("finish1"):
        finish1()
    wait_some(d_recv, group - 1, send_sems.at[11])


def fused(devices, pair, residue_mask, norm_gain, proj_weight, gate_weight, mix_gain, out_weight):
    rows, total, chans = pair.shape
    hidden = mix_gain.shape[1]
    group = devices // HALVES
    own = hidden // group
    cols = total // HALVES
    spots = rows * cols
    pairs = rows // 2
    half_rows = group * pairs * own
    hbm = pl.BlockSpec(memory_space=pltpu.HBM)
    params = (norm_gain, proj_weight, gate_weight, mix_gain, out_weight)
    operands = [
        pltpu.with_memory_space_constraint(v, pltpu.HBM) for v in (pair, residue_mask, *params)
    ]
    return pl.pallas_call(
        functools.partial(fused_kernel, devices),
        out_shape=pltpu.VMEM(pair.shape, BF16),
        in_specs=[hbm] * 7,
        out_specs=pl.BlockSpec(memory_space=pltpu.VMEM),
        scratch_shapes=[
            pltpu.VMEM(pair.shape, BF16),
            pltpu.SMEM(residue_mask.shape, jnp.int32),
            *(pltpu.VMEM(p.shape, p.dtype) for p in params),
            pltpu.VMEM((1, total), F32),
            pltpu.VMEM((devices, 1, total), F32),
            pltpu.VMEM((group, 2, rows * own, total), BF16),
            pltpu.VMEM((group, 2, rows * own, total), BF16),
            pltpu.VMEM((group, rows * own, total), BF16),
            pltpu.VMEM((rows, cols, chans), BF16),
            pltpu.VMEM((2, group, pairs * own, total), BF16),
            pltpu.VMEM((2, group, pairs * own, total), BF16),
            pltpu.VMEM((2, group, 2, pairs * own, total), BF16),
            pltpu.VMEM((2, group, 2, pairs * own, total), BF16),
            pltpu.VMEM((2, group, pairs * own, total), BF16),
            pltpu.VMEM((chans, spots), BF16),
            pltpu.VMEM((group, rows * own, total), BF16),
            pltpu.VMEM((group, rows * own, total), BF16),
            pltpu.VMEM((2, 4 * hidden, chans), BF16),
            pltpu.VMEM((chans, chans), BF16),
            pltpu.VMEM((chans, hidden), BF16),
            pltpu.VMEM((2, hidden, total), F32),
            pltpu.VMEM((chans, total), F32),
            pltpu.VMEM((2, 1, spots), F32),
            pltpu.VMEM((rows, total, chans), BF16),
            pltpu.VMEM((chans, spots), BF16),
            pltpu.VMEM((2, chans, spots), BF16),
            pltpu.VMEM((2, chans, spots), BF16),
            pltpu.VMEM((2, chans, spots), F32),
            pltpu.VMEM((2, spots, chans), BF16),
            pltpu.VMEM((2, spots, chans), F32),
            pltpu.VMEM((2, group * rows * own, total), F32),
            pltpu.VMEM((group * rows * own, total), F32),
            pltpu.VMEM((own, total, 2 * total), BF16),
            pltpu.VMEM((2, half_rows, total), F32),
            pltpu.VMEM((2 * half_rows, total), F32),
            pltpu.VMEM((2 * half_rows, total), F32),
            pltpu.VMEM((2 * half_rows, total), F32),
            pltpu.VMEM((cols * own, total), F32),
            pltpu.SemaphoreType.DMA((12,)),
            pltpu.SemaphoreType.DMA((12,)),
            pltpu.SemaphoreType.DMA((7,)),
        ],
        compiler_params=pltpu.CompilerParams(
            collective_id=0, has_side_effects=True, vmem_limit_bytes=16777216
        ),
        name="triangles",
    )(*operands)


def panels(rows, mask_rows, mask_all, gain, weight):
    hidden = weight.shape[1] // 4
    mask_float = mask_all.astype(F32)
    normed = (normalize(rows.astype(F32), 2) * gain).astype(BF16)
    proj = jnp.einsum("rnc,ch->hrn", normed, weight, preferred_element_type=F32)
    scale = mask_rows.astype(F32)[:, None] * mask_float[None, :]
    left = (jax.nn.sigmoid(proj[:hidden]) * proj[hidden : 2 * hidden] * scale).astype(BF16)
    right = (jax.nn.sigmoid(proj[2 * hidden : 3 * hidden]) * proj[3 * hidden :] * scale).astype(
        BF16
    )
    return (normed, left, right)


def triangle(rows, mask_rows, mask_all, gain, weight, gate_w, tri_gain, out_w, second):
    normed, left, right = panels(rows, mask_rows, mask_all, gain, weight)
    left = lax.all_to_all(left, "dap", split_axis=0, concat_axis=1, tiled=True)
    right = lax.all_to_all(right, "dap", split_axis=0, concat_axis=1, tiled=True)
    spec = "cki,ckj->cij" if second else "cik,cjk->cij"
    tri = jnp.einsum(spec, left, right, preferred_element_type=F32).astype(BF16)
    tri = lax.all_to_all(tri, "dap", split_axis=1, concat_axis=0, tiled=True)
    gate = jax.nn.sigmoid(jnp.einsum("rnc,cd->rnd", normed, gate_w, preferred_element_type=F32))
    tri_normed = (normalize(tri.astype(F32), 0) * tri_gain[:, None, None]).astype(BF16)
    out = jnp.einsum("hrn,hc->rnc", tri_normed, out_w, preferred_element_type=F32)
    return (rows.astype(F32) + gate * out).astype(BF16)


def by_collectives(pair, residue_mask, *params):
    mask_all = lax.all_gather(residue_mask, "dap", axis=0, tiled=True)
    state = pair
    for layer in range(2):
        gain, weight, gate_w, tri_gain, out_w = (p[layer] for p in params)
        state = triangle(
            state, residue_mask, mask_all, gain, weight, gate_w, tri_gain, out_w, layer == 1
        )
    return state


def solution(mesh):
    devices = mesh.shape["dap"]

    def body(pair, residue_mask, norm_gain, proj_weight, gate_weight, mix_gain, out_weight):
        args = (pair, residue_mask, norm_gain, proj_weight, gate_weight, mix_gain, out_weight)
        group = devices // HALVES
        own = mix_gain.shape[1] // group
        rows, total, chans = pair.shape
        whole = group * HALVES == devices and group & (group - 1) == 0
        whole = whole and own * group == chans == mix_gain.shape[1] == total == 128
        if whole and own == 8 and rows == 4:
            return fused(devices, *args)
        return by_collectives(*args)

    return jax.shard_map(
        body,
        mesh=mesh,
        in_specs=(P("dap", None, None), P("dap"), P(), P(), P(), P(), P()),
        out_specs=P("dap", None, None),
        check_vma=False,
    )
```

```python
import contextlib
import functools

import jax
import jax.numpy as jnp
from jax import lax
from jax.experimental import pallas as pl
from jax.experimental.pallas import tpu as pltpu
from jax.sharding import PartitionSpec as P

EPS = 1e-05
F32 = jnp.float32
BF16 = jnp.bfloat16
MESH = pl.DeviceIdType.MESH
HALVES = 2


def normalize(values, axis):
    center = values - jnp.mean(values, axis=axis, keepdims=True)
    spread = jnp.mean(center * center, axis=axis, keepdims=True)
    return center * lax.rsqrt(spread + EPS)


def dot(a, b, dims):
    return lax.dot_general(a, b, ((dims[:1], dims[1:]), ((), ())), preferred_element_type=F32)


def mark(name):
    return contextlib.nullcontext()


def fused_kernel(
    devices,
    pair_hbm,
    mask_hbm,
    norm_hbm,
    proj_hbm,
    gate_hbm,
    mix_hbm,
    outw_hbm,
    out_ref,
    pair_ref,
    mask_ref,
    norm_ref,
    proj_ref,
    gate_ref,
    mix_ref,
    outw_ref,
    mask_send,
    mask_recv,
    a_send,
    a_near,
    a_far,
    pair_far,
    b_send,
    b_recv,
    c_send,
    c_near,
    c_far,
    back_recv,
    d_send,
    d_recv,
    weight_s,
    gatew_s,
    outw_s,
    mixg_s,
    normg_s,
    scale_s,
    normed_s,
    normed1_s,
    zt_s,
    z1t_s,
    gate0_s,
    z1_s,
    gate1_s,
    left_s,
    right_s,
    rhs_s,
    flat_s,
    lhs1_s,
    own1_s,
    far1_s,
    flat1_s,
    send_sems,
    recv_sems,
    load_sems,
):
    sources = (pair_hbm, proj_hbm, mask_hbm, norm_hbm, gate_hbm, mix_hbm, outw_hbm)
    places = (pair_ref, proj_ref, mask_ref, norm_ref, gate_ref, mix_ref, outw_ref)
    loads = [
        pltpu.make_async_copy(source, place, load_sems.at[slot])
        for slot, (source, place) in enumerate(zip(sources, places))
    ]
    for load in loads:
        load.start()
    rows, total, chans = pair_ref.shape
    hidden = mix_ref.shape[1]
    group = devices // HALVES
    own = hidden // group
    cols = total // HALVES
    spots = rows * cols
    pairs = rows // 2
    me = lax.axis_index("dap")
    half = me // group
    spot = lax.rem(me, group)
    partner = lax.rem(me + group, devices)
    zone = me * 4 // devices
    flip = jnp.where((zone == 0) | (zone == 3), group // 2, 0)
    near_cols = pl.ds(pl.multiple_of(half * cols, cols), cols)
    far_cols = pl.ds(pl.multiple_of((1 - half) * cols, cols), cols)

    barrier = pltpu.get_barrier_semaphore()

    def greet(step, carry):
        peer = me ^ (devices - step)
        pl.semaphore_signal(barrier, inc=1, device_id=(peer,), device_id_type=MESH)
        return carry

    lax.fori_loop(1, devices, greet, 0)

    def push(src, dst, slot, peer):
        pltpu.make_async_remote_copy(
            src_ref=src,
            dst_ref=dst,
            send_sem=send_sems.at[slot],
            recv_sem=recv_sems.at[slot],
            device_id=(peer,),
            device_id_type=MESH,
        ).start()

    def push_near(src, dst, slot):
        def one(step, carry):
            bits = group - step
            push(src(spot ^ bits), dst, slot, me ^ bits)
            return carry

        lax.fori_loop(1, group, one, 0, unroll=True)

    def push_far(src, dst, slot, turn_by=0):
        def one(step, carry):
            bits = (group - step) ^ turn_by
            push(src(spot ^ bits), dst, slot, me ^ (group + bits))
            return carry

        lax.fori_loop(1, group + 1, one, 0, unroll=True)

    def push_all(src, dst, slot):
        def one(step, carry):
            push(src, dst, slot, me ^ (devices - step))
            return carry

        lax.fori_loop(1, devices, one, 0, unroll=True)

    def wait_all(buf, sem):
        pltpu.make_async_copy(buf, buf, sem).wait()

    def wait_some(buf, count, sem):
        part = buf.at[pl.ds(0, count)]
        pltpu.make_async_copy(part, part, sem).wait()

    def lanes_of(parts):
        return jnp.concatenate(parts, axis=1)

    def panels_of(layer, normed, dims, side):
        at = 2 * side * hidden
        gate = dot(weight_s[layer, at : at + hidden], normed, dims)
        value = dot(weight_s[layer, at + hidden : at + 2 * hidden], normed, dims)
        return jax.nn.sigmoid(gate) * value

    def make_panels0():
        for pair in range(pairs):
            normed = normed_s[2 * pair : 2 * pair + 2].reshape(2 * total, chans)
            for side in range(2):
                panel = panels_of(0, normed, (1, 1), side)
                parts = [
                    (panel[:, r * total : (r + 1) * total] * mask_ref[2 * pair + r].astype(F32))
                    for r in range(2)
                ]
                tile = jnp.concatenate([p.reshape(group, own, total) for p in parts], axis=1)
                at = pl.ds(2 * own * pair, 2 * own)
                a_send[:, side, at, :] = tile.astype(BF16)

    def make_gate0(part, normed):
        gate0_s[part] = jax.nn.sigmoid(dot(gatew_s[...], normed, (1, 1)))

    def turn(values):
        return values.astype(F32).T.astype(BF16)

    def set_scale(part, owner, column_mask, doubled):
        entry = [
            jnp.sum(jnp.where(lane == owner * rows + r, column_mask, 0.0), axis=1, keepdims=True)
            for r in range(rows)
        ]
        scale_s[part] = lanes_of(
            [
                jnp.where(lane < cols, entry[2 * p], entry[2 * p + 1]) * doubled
                for p in range(pairs)
            ]
        )

    def outgoing(part, panel):
        left_s[part] = panel.astype(F32).reshape(group * rows * own, total)
        for c in range(own):
            left = jnp.concatenate(
                [
                    lanes_of(
                        [
                            left_s[part, pl.ds((2 * p + r) * own + c, group, stride=rows * own), :]
                            for r in range(2)
                        ]
                    )
                    for p in range(pairs)
                ],
                axis=0,
            ).astype(BF16)
            tri = dot(left, rhs_s[c], (1, 1))
            for p in range(pairs):
                flat_s[part, pl.ds(p * own + c, group, stride=pairs * own), :] = tri[
                    p * group : (p + 1) * group
                ]
        b_send[part] = flat_s[part].reshape(group, pairs * own, total).astype(BF16)

    def send_b(part):
        push_near(lambda at: b_send.at[part, at], b_recv.at[part, spot], 5 + part)
        b_recv[part, spot] = b_send[part, spot]

    def finish0(part):
        got = b_recv[part].astype(F32)
        tri = lanes_of(
            [got[:, p * own : (p + 1) * own].reshape(hidden, total) for p in range(pairs)]
        )
        gain = mixg_s[0]
        tri_normed = (normalize(tri, 0) * lanes_of([gain] * pairs)).astype(BF16)
        out = dot(outw_s[...], tri_normed, (1, 0))
        new = (zt_s[part].astype(F32) + gate0_s[part] * out).astype(BF16)
        z1t_s[part] = new
        normed = (normalize(new.astype(F32), 0) * lanes_of([normg_s[...]] * pairs)).astype(BF16)
        if part == 0:
            normed1_s[...] = normed
        for side in (1, 0):
            panel = panels_of(1, normed, (1, 0), side) * scale_s[part]
            tile = jnp.concatenate(
                [
                    panel[:, p * total : (p + 1) * total].reshape(group, own, total)
                    for p in range(pairs)
                ],
                axis=1,
            )
            c_send[part, :, side] = tile.astype(BF16)
            if side == 1:
                push_far(
                    lambda at: c_send.at[part, at, 1], c_far.at[part, spot], 9 + part, flip
                )

    def send_c(part):
        push_near(lambda at: c_send.at[part, at], c_near.at[part, spot], 7 + part)
        c_near[part, spot] = c_send[part, spot]

    def natural(part, normed):
        gate1_s[part] = jax.nn.sigmoid(dot(normed, gate_ref[1], (1, 0)))

    def unpack1(part):
        size = group * pairs * own
        at = pl.ds(part * size, size)
        near = c_near[part].astype(F32)
        lhs1_s[at, :] = near[:, 0].reshape(size, total)
        own1_s[at, :] = near[:, 1].reshape(size, total)
        far1_s[pl.ds((1 - part) * size, size), :] = c_far[part].astype(F32).reshape(size, total)

    def incoming():
        count = HALVES * group * pairs
        low = lane < cols
        for c in range(own):
            pick = pl.ds(c, count, stride=own)
            left = lhs1_s[pick, :].astype(BF16)
            right = lanes_of([own1_s[pick, :], far1_s[pick, :]]).astype(BF16)
            prod = dot(left, right, (0, 0))
            straight = jnp.where(low, prod[:cols, :total], prod[cols:, total:])
            crossed = jnp.where(low, prod[:cols, total:], prod[cols:, :total])
            tri = straight + pltpu.roll(crossed, cols, 1)
            flat1_s[pl.ds(c, cols, stride=own), :] = tri
        d_send[...] = flat1_s[...].reshape(group, rows * own, total).astype(BF16)

    def finish1():
        got = d_recv[...].astype(F32)
        for r in range(rows):
            tri = got[:, r * own : (r + 1) * own].reshape(hidden, total)
            tri_normed = (normalize(tri, 0) * mixg_s[1]).astype(BF16)
            out = dot(tri_normed, outw_ref[1], (0, 0))
            block = pl.ds(r * cols, cols)
            for part, place in enumerate((near_cols, far_cols)):
                piece = out[part * cols : (part + 1) * cols]
                new = z1_s[part, block, :].astype(F32) + gate1_s[part, block, :] * piece
                out_ref[r, place, :] = new.astype(BF16)

    lane = lax.broadcasted_iota(jnp.int32, (1, total), 1)
    with mark("load"):
        for load in loads:
            load.wait()
    with mark("panels0"):
        mask_row = jnp.zeros((1, total), F32)
        for r in range(rows):
            mask_row = mask_row + jnp.where(lane == me * rows + r, mask_ref[r].astype(F32), 0.0)
        mask_send[...] = mask_row
        weight_s[0] = turn(proj_ref[0])
        z = pair_ref[...].reshape(rows * total, chans).astype(F32)
        normed = (normalize(z, 1) * norm_ref[pl.ds(0, 1), :]).astype(BF16)
        normed_s[...] = normed.reshape(rows, total, chans)
        make_panels0()
    with mark("barrier"):
        pl.semaphore_wait(barrier, devices - 1)
    with mark("sendA"):
        push_all(mask_send, mask_recv.at[me], 0)
        push_near(lambda at: a_send.at[at], a_near.at[spot], 1)
        push_far(lambda at: a_send.at[at, 0], a_far.at[spot], 2, flip)
        mask_recv[me] = mask_send[...]
        a_near[spot] = a_send[spot]
    with mark("idleA"):
        gatew_s[...] = turn(gate_ref[0])
        outw_s[...] = turn(outw_ref[0])
        weight_s[1] = turn(proj_ref[1])
        for layer in range(2):
            mixg_s[layer] = jnp.broadcast_to(mix_ref[pl.ds(layer, 1), :], (total, hidden)).T
        normg_s[...] = jnp.broadcast_to(norm_ref[pl.ds(1, 1), :], (total, chans)).T
        rhs_s[...] = jnp.zeros(rhs_s.shape, BF16)
        zt_s[0] = turn(pair_ref[:, near_cols, :].reshape(spots, chans))
        make_gate0(0, normed_s[:, near_cols, :].reshape(spots, chans))
    with mark("waitmask"):
        wait_some(mask_recv, devices - 1, recv_sems.at[0])
    with mark("masks"):
        column_mask = jnp.sum(mask_recv[...], axis=0)
        doubled = jnp.where(lane // cols == half, column_mask, pltpu.roll(column_mask, cols, 1))
        set_scale(0, me, column_mask, doubled)
        set_scale(1, partner, column_mask, doubled)
    with mark("waitAnear"):
        wait_some(a_near, group - 1, recv_sems.at[1])
    with mark("out0"):
        right_s[...] = a_near[:, 1].astype(F32).reshape(group * rows * own, total)
        for c in range(own):
            right = (right_s[pl.ds(c, cols, stride=own), :] * column_mask).astype(BF16)
            rhs_s[c, 0:cols, 0:total] = right
            rhs_s[c, cols : 2 * cols, total : 2 * total] = right
        outgoing(0, a_near[:, 0])
    with mark("sendB0"):
        send_b(0)
        push(pair_ref.at[:, far_cols, :], pair_far, 3, partner)
    with mark("waitAfar"):
        wait_all(a_far, recv_sems.at[2])
    with mark("out1"):
        outgoing(1, a_far[...])
    with mark("sendB1"):
        send_b(1)
    with mark("waitB0"):
        wait_some(b_recv.at[0], group - 1, recv_sems.at[5])
    with mark("fin0"):
        finish0(0)
    with mark("sendC0"):
        send_c(0)
    with mark("waitpair"):
        wait_all(pair_far, recv_sems.at[3])
    with mark("pair"):
        z = pair_far[...].reshape(spots, chans)
        zt_s[1] = turn(z)
        make_gate0(1, (normalize(z.astype(F32), 1) * norm_ref[pl.ds(0, 1), :]).astype(BF16))
    with mark("waitB1"):
        wait_some(b_recv.at[1], group - 1, recv_sems.at[6])
    with mark("fin1"):
        finish0(1)
    with mark("sendC1"):
        send_c(1)
    with mark("nat0"):
        z1_s[0] = z1t_s[0].astype(F32).T.astype(BF16)
        natural(0, normed1_s[...].astype(F32).T.astype(BF16))
    with mark("waitC0"):
        wait_some(c_near.at[0], group - 1, recv_sems.at[7])
        wait_all(c_far.at[0], recv_sems.at[9])
    with mark("back"):
        push(z1t_s.at[1], back_recv, 4, partner)
    with mark("unpack0"):
        unpack1(0)
    with mark("waitC1"):
        wait_some(c_near.at[1], group - 1, recv_sems.at[8])
        wait_all(c_far.at[1], recv_sems.at[10])
    with mark("in"):
        unpack1(1)
        incoming()
    with mark("sendD"):
        push_near(lambda at: d_send.at[at], d_recv.at[spot], 11)
        d_recv[spot] = d_send[spot]
    with mark("waitback"):
        wait_all(back_recv, recv_sems.at[4])
    with mark("nat1"):
        z = back_recv[...].astype(F32).T
        z1_s[1] = z.astype(BF16)
        natural(1, (normalize(z, 1) * norm_ref[pl.ds(1, 1), :]).astype(BF16))
        wait_some(mask_recv, devices - 1, send_sems.at[0])
        wait_some(a_near, group - 1, send_sems.at[1])
        wait_all(a_far, send_sems.at[2])
        wait_all(pair_far, send_sems.at[3])
        wait_all(back_recv, send_sems.at[4])
        wait_all(c_far.at[0], send_sems.at[9])
        for part in range(2):
            wait_some(b_recv.at[part], group - 1, send_sems.at[5 + part])
            wait_some(c_near.at[part], group - 1, send_sems.at[7 + part])
        pass
        wait_all(c_far.at[1], send_sems.at[10])
    with mark("waitD"):
        wait_some(d_recv, group - 1, recv_sems.at[11])
    with mark("finish1"):
        finish1()
    wait_some(d_recv, group - 1, send_sems.at[11])


def fused(devices, pair, residue_mask, norm_gain, proj_weight, gate_weight, mix_gain, out_weight):
    rows, total, chans = pair.shape
    hidden = mix_gain.shape[1]
    group = devices // HALVES
    own = hidden // group
    cols = total // HALVES
    spots = rows * cols
    pairs = rows // 2
    half_rows = group * pairs * own
    hbm = pl.BlockSpec(memory_space=pltpu.HBM)
    params = (norm_gain, proj_weight, gate_weight, mix_gain, out_weight)
    operands = [
        pltpu.with_memory_space_constraint(v, pltpu.HBM) for v in (pair, residue_mask, *params)
    ]
    return pl.pallas_call(
        functools.partial(fused_kernel, devices),
        out_shape=pltpu.VMEM(pair.shape, BF16),
        in_specs=[hbm] * 7,
        out_specs=pl.BlockSpec(memory_space=pltpu.VMEM),
        scratch_shapes=[
            pltpu.VMEM(pair.shape, BF16),
            pltpu.SMEM(residue_mask.shape, jnp.int32),
            *(pltpu.VMEM(p.shape, p.dtype) for p in params),
            pltpu.VMEM((1, total), F32),
            pltpu.VMEM((devices, 1, total), F32),
            pltpu.VMEM((group, 2, rows * own, total), BF16),
            pltpu.VMEM((group, 2, rows * own, total), BF16),
            pltpu.VMEM((group, rows * own, total), BF16),
            pltpu.VMEM((rows, cols, chans), BF16),
            pltpu.VMEM((2, group, pairs * own, total), BF16),
            pltpu.VMEM((2, group, pairs * own, total), BF16),
            pltpu.VMEM((2, group, 2, pairs * own, total), BF16),
            pltpu.VMEM((2, group, 2, pairs * own, total), BF16),
            pltpu.VMEM((2, group, pairs * own, total), BF16),
            pltpu.VMEM((chans, spots), BF16),
            pltpu.VMEM((group, rows * own, total), BF16),
            pltpu.VMEM((group, rows * own, total), BF16),
            pltpu.VMEM((2, 4 * hidden, chans), BF16),
            pltpu.VMEM((chans, chans), BF16),
            pltpu.VMEM((chans, hidden), BF16),
            pltpu.VMEM((2, hidden, total), F32),
            pltpu.VMEM((chans, total), F32),
            pltpu.VMEM((2, 1, spots), F32),
            pltpu.VMEM((rows, total, chans), BF16),
            pltpu.VMEM((chans, spots), BF16),
            pltpu.VMEM((2, chans, spots), BF16),
            pltpu.VMEM((2, chans, spots), BF16),
            pltpu.VMEM((2, chans, spots), F32),
            pltpu.VMEM((2, spots, chans), BF16),
            pltpu.VMEM((2, spots, chans), F32),
            pltpu.VMEM((2, group * rows * own, total), F32),
            pltpu.VMEM((group * rows * own, total), F32),
            pltpu.VMEM((own, total, 2 * total), BF16),
            pltpu.VMEM((2, half_rows, total), F32),
            pltpu.VMEM((2 * half_rows, total), F32),
            pltpu.VMEM((2 * half_rows, total), F32),
            pltpu.VMEM((2 * half_rows, total), F32),
            pltpu.VMEM((cols * own, total), F32),
            pltpu.SemaphoreType.DMA((12,)),
            pltpu.SemaphoreType.DMA((12,)),
            pltpu.SemaphoreType.DMA((7,)),
        ],
        compiler_params=pltpu.CompilerParams(
            collective_id=0, has_side_effects=True, vmem_limit_bytes=16777216
        ),
        name="triangles",
    )(*operands)


def panels(rows, mask_rows, mask_all, gain, weight):
    hidden = weight.shape[1] // 4
    mask_float = mask_all.astype(F32)
    normed = (normalize(rows.astype(F32), 2) * gain).astype(BF16)
    proj = jnp.einsum("rnc,ch->hrn", normed, weight, preferred_element_type=F32)
    scale = mask_rows.astype(F32)[:, None] * mask_float[None, :]
    left = (jax.nn.sigmoid(proj[:hidden]) * proj[hidden : 2 * hidden] * scale).astype(BF16)
    right = (jax.nn.sigmoid(proj[2 * hidden : 3 * hidden]) * proj[3 * hidden :] * scale).astype(
        BF16
    )
    return (normed, left, right)


def triangle(rows, mask_rows, mask_all, gain, weight, gate_w, tri_gain, out_w, second):
    normed, left, right = panels(rows, mask_rows, mask_all, gain, weight)
    left = lax.all_to_all(left, "dap", split_axis=0, concat_axis=1, tiled=True)
    right = lax.all_to_all(right, "dap", split_axis=0, concat_axis=1, tiled=True)
    spec = "cki,ckj->cij" if second else "cik,cjk->cij"
    tri = jnp.einsum(spec, left, right, preferred_element_type=F32).astype(BF16)
    tri = lax.all_to_all(tri, "dap", split_axis=1, concat_axis=0, tiled=True)
    gate = jax.nn.sigmoid(jnp.einsum("rnc,cd->rnd", normed, gate_w, preferred_element_type=F32))
    tri_normed = (normalize(tri.astype(F32), 0) * tri_gain[:, None, None]).astype(BF16)
    out = jnp.einsum("hrn,hc->rnc", tri_normed, out_w, preferred_element_type=F32)
    return (rows.astype(F32) + gate * out).astype(BF16)


def by_collectives(pair, residue_mask, *params):
    mask_all = lax.all_gather(residue_mask, "dap", axis=0, tiled=True)
    state = pair
    for layer in range(2):
        gain, weight, gate_w, tri_gain, out_w = (p[layer] for p in params)
        state = triangle(
            state, residue_mask, mask_all, gain, weight, gate_w, tri_gain, out_w, layer == 1
        )
    return state


def solution(mesh):
    devices = mesh.shape["dap"]

    def body(pair, residue_mask, norm_gain, proj_weight, gate_weight, mix_gain, out_weight):
        args = (pair, residue_mask, norm_gain, proj_weight, gate_weight, mix_gain, out_weight)
        group = devices // HALVES
        own = mix_gain.shape[1] // group
        rows, total, chans = pair.shape
        whole = group * HALVES == devices and group & (group - 1) == 0
        whole = whole and own * group == chans == mix_gain.shape[1] == total == 128
        if whole and own == 8 and rows == 4:
            return fused(devices, *args)
        return by_collectives(*args)

    return jax.shard_map(
        body,
        mesh=mesh,
        in_specs=(P("dap", None, None), P("dap"), P(), P(), P(), P(), P()),
        out_specs=P("dap", None, None),
        check_vma=False,
    )
```

```python
import contextlib
import functools

import jax
import jax.numpy as jnp
from jax import lax
from jax.experimental import pallas as pl
from jax.experimental.pallas import tpu as pltpu
from jax.sharding import PartitionSpec as P

EPS = 1e-05
F32 = jnp.float32
BF16 = jnp.bfloat16
MESH = pl.DeviceIdType.MESH
HALVES = 2
PAD = 8


def normalize(values, axis):
    center = values - jnp.mean(values, axis=axis, keepdims=True)
    spread = jnp.mean(center * center, axis=axis, keepdims=True)
    return center * lax.rsqrt(spread + EPS)


def normalize_down(values):
    moved = values - values[:1]
    center = jnp.mean(moved, axis=0, keepdims=True)
    spread = jnp.mean(moved * moved, axis=0, keepdims=True) - center * center
    return (moved - center) * lax.rsqrt(jnp.maximum(spread, 0.0) + EPS)


def dot(a, b, dims):
    return lax.dot_general(a, b, ((dims[:1], dims[1:]), ((), ())), preferred_element_type=F32)


def mark(name):
    return contextlib.nullcontext()


def fused_kernel(
    devices,
    pair_hbm,
    mask_hbm,
    norm_hbm,
    proj_hbm,
    gate_hbm,
    mix_hbm,
    outw_hbm,
    out_ref,
    pair_ref,
    mask_ref,
    norm_ref,
    proj_ref,
    gate_ref,
    mix_ref,
    outw_ref,
    mask_send,
    mask_recv,
    a_send,
    a_near,
    a_far,
    pair_far,
    b_send,
    b_recv,
    c_send,
    c_near,
    c_far,
    back_recv,
    d_send,
    d_recv,
    weight_s,
    gatew_s,
    outw_s,
    mixg_s,
    normg_s,
    scale_s,
    normed_s,
    normed1_s,
    zt_s,
    z1t_s,
    gate0_s,
    z1_s,
    gate1_s,
    left_s,
    right_s,
    rhs_s,
    flat_s,
    lhs1_s,
    own1_s,
    far1_s,
    flat1_s,
    send_sems,
    recv_sems,
    load_sems,
):
    rows, total, chans = pair_ref.shape
    hidden = mix_ref.shape[1]
    group = devices // HALVES
    own = hidden // group
    cols = total // HALVES
    spots = rows * cols
    pairs = rows // 2
    step = rows * own + PAD
    me = lax.axis_index("dap")
    half = me // group
    spot = lax.rem(me, group)
    partner = lax.rem(me + group, devices)
    zone = me * 4 // devices
    flip = jnp.where((zone == 0) | (zone == 3), group // 2, 0)
    near_cols = pl.ds(pl.multiple_of(half * cols, cols), cols)
    far_cols = pl.ds(pl.multiple_of((1 - half) * cols, cols), cols)

    barrier = pltpu.get_barrier_semaphore()

    def greet(step, carry):
        peer = me ^ (devices - step)
        pl.semaphore_signal(barrier, inc=1, device_id=(peer,), device_id_type=MESH)
        return carry

    lax.fori_loop(1, devices, greet, 0, unroll=True)

    sources = (pair_hbm, proj_hbm, mask_hbm, norm_hbm, gate_hbm, mix_hbm, outw_hbm)
    places = (pair_ref, proj_ref, mask_ref, norm_ref, gate_ref, mix_ref, outw_ref)
    loads = [
        pltpu.make_async_copy(source, place, load_sems.at[slot])
        for slot, (source, place) in enumerate(zip(sources, places))
    ]
    for load in loads:
        load.start()
    def push(src, dst, slot, peer):
        pltpu.make_async_remote_copy(
            src_ref=src,
            dst_ref=dst,
            send_sem=send_sems.at[slot],
            recv_sem=recv_sems.at[slot],
            device_id=(peer,),
            device_id_type=MESH,
        ).start()

    def push_near(src, dst, slot):
        def one(step, carry):
            bits = group - step
            push(src(spot ^ bits), dst, slot, me ^ bits)
            return carry

        lax.fori_loop(1, group, one, 0, unroll=True)

    def push_far(src, dst, slot, turn_by=0):
        def one(step, carry):
            bits = (group - step) ^ turn_by
            push(src(spot ^ bits), dst, slot, me ^ (group + bits))
            return carry

        lax.fori_loop(1, group + 1, one, 0, unroll=True)

    def push_all(src, dst, slot):
        def one(step, carry):
            push(src, dst, slot, me ^ (devices - step))
            return carry

        lax.fori_loop(1, devices, one, 0, unroll=True)

    def wait_all(buf, sem):
        pltpu.make_async_copy(buf, buf, sem).wait()

    def wait_some(buf, count, sem):
        part = buf.at[pl.ds(0, count)]
        pltpu.make_async_copy(part, part, sem).wait()

    def lanes_of(parts):
        return jnp.concatenate(parts, axis=1)

    def panels_of(layer, normed, dims, side):
        at = 2 * side * hidden
        gate = dot(weight_s[layer, at : at + hidden], normed, dims)
        value = dot(weight_s[layer, at + hidden : at + 2 * hidden], normed, dims)
        return jax.nn.sigmoid(gate) * value

    def make_panels0():
        for pair in range(pairs):
            normed = normed_s[2 * pair : 2 * pair + 2].reshape(2 * total, chans)
            for side in range(2):
                panel = panels_of(0, normed, (1, 1), side)
                parts = [
                    (panel[:, r * total : (r + 1) * total] * mask_ref[2 * pair + r].astype(F32))
                    for r in range(2)
                ]
                tile = jnp.concatenate([p.reshape(group, own, total) for p in parts], axis=1)
                at = pl.ds(2 * own * pair, 2 * own)
                a_send[:, side, at, :] = tile.astype(BF16)

    def make_gate0(part, normed):
        gate0_s[part] = jax.nn.sigmoid(dot(gatew_s[...], normed, (1, 1)))

    def turn(values):
        return values.astype(F32).T.astype(BF16)

    def set_scale(part, owner, column_mask, doubled):
        entry = [
            jnp.sum(jnp.where(lane == owner * rows + r, column_mask, 0.0), axis=1, keepdims=True)
            for r in range(rows)
        ]
        scale_s[part] = lanes_of(
            [
                jnp.where(lane < cols, entry[2 * p], entry[2 * p + 1]) * doubled
                for p in range(pairs)
            ]
        )

    def outgoing(part, panel):
        for p in range(group):
            left_s[part, p * step : p * step + rows * own, :] = panel[p].astype(F32)
        for c in range(own):
            left = jnp.concatenate(
                [
                    lanes_of(
                        [
                            left_s[part, pl.ds((2 * p + r) * own + c, group, stride=step), :]
                            for r in range(2)
                        ]
                    )
                    for p in range(pairs)
                ],
                axis=0,
            ).astype(BF16)
            tri = dot(left, rhs_s[c], (1, 1))
            for p in range(pairs):
                flat_s[part, pl.ds(p * own + c, group, stride=pairs * own), :] = tri[
                    p * group : (p + 1) * group
                ]
        b_send[part] = flat_s[part].reshape(group, pairs * own, total).astype(BF16)

    def send_b(part):
        push_near(lambda at: b_send.at[part, at], b_recv.at[part, spot], 5 + part)
        b_recv[part, spot] = b_send[part, spot]

    def finish0(part):
        got = b_recv[part].astype(F32)
        tri = lanes_of(
            [got[:, p * own : (p + 1) * own].reshape(hidden, total) for p in range(pairs)]
        )
        gain = mixg_s[0]
        tri_normed = (normalize_down(tri) * lanes_of([gain] * pairs)).astype(BF16)
        out = lanes_of(
            [
                dot(outw_s[...], tri_normed[:, p * total : (p + 1) * total], (1, 0))
                for p in range(pairs)
            ]
        )
        new = (zt_s[part].astype(F32) + gate0_s[part] * out).astype(BF16)
        z1t_s[part] = new
        normed = (normalize_down(new.astype(F32)) * lanes_of([normg_s[...]] * pairs)).astype(BF16)
        if part == 0:
            normed1_s[...] = normed
        for side in (1, 0):
            panel = panels_of(1, normed, (1, 0), side) * scale_s[part]
            tile = jnp.concatenate(
                [
                    panel[:, p * total : (p + 1) * total].reshape(group, own, total)
                    for p in range(pairs)
                ],
                axis=1,
            )
            c_send[part, :, side] = tile.astype(BF16)
            if side == 1:
                push_far(
                    lambda at: c_send.at[part, at, 1], c_far.at[part, spot], 9 + part, flip
                )

    def send_c(part):
        push_near(lambda at: c_send.at[part, at], c_near.at[part, spot], 7 + part)
        c_near[part, spot] = c_send[part, spot]

    def natural(part, normed):
        gate1_s[part] = jax.nn.sigmoid(dot(normed, gate_ref[1], (1, 0)))

    def unpack1(part):
        size = group * pairs * own
        at = pl.ds(part * size, size)
        near = c_near[part].astype(F32)
        lhs1_s[at, :] = near[:, 0].reshape(size, total)
        own1_s[at, :] = near[:, 1].reshape(size, total)
        far1_s[pl.ds((1 - part) * size, size), :] = c_far[part].astype(F32).reshape(size, total)

    def incoming():
        count = HALVES * group * pairs
        low = lane < cols
        for c in range(own):
            pick = pl.ds(c, count, stride=own)
            left = lhs1_s[pick, :].astype(BF16).T
            right = lanes_of([own1_s[pick, :], far1_s[pick, :]]).astype(BF16)
            prod = dot(left, right, (1, 0))
            straight = jnp.where(low, prod[:cols, :total], prod[cols:, total:])
            crossed = jnp.where(low, prod[:cols, total:], prod[cols:, :total])
            tri = straight + pltpu.roll(crossed, cols, 1)
            flat1_s[pl.ds(c, cols, stride=own), :] = tri
        d_send[...] = flat1_s[...].reshape(group, rows * own, total).astype(BF16)

    def finish1():
        got = d_recv[...].astype(F32)
        for r in range(rows):
            tri = got[:, r * own : (r + 1) * own].reshape(hidden, total)
            tri_normed = (normalize_down(tri) * mixg_s[1]).astype(BF16)
            out = dot(tri_normed, outw_ref[1], (0, 0))
            block = pl.ds(r * cols, cols)
            for part, place in enumerate((near_cols, far_cols)):
                piece = out[part * cols : (part + 1) * cols]
                new = z1_s[part, block, :].astype(F32) + gate1_s[part, block, :] * piece
                out_ref[r, place, :] = new.astype(BF16)

    lane = lax.broadcasted_iota(jnp.int32, (1, total), 1)
    with mark("load"):
        for load in loads:
            load.wait()
    with mark("panels0"):
        mask_row = jnp.zeros((1, total), F32)
        for r in range(rows):
            mask_row = mask_row + jnp.where(lane == me * rows + r, mask_ref[r].astype(F32), 0.0)
        mask_send[...] = mask_row
        weight_s[0] = turn(proj_ref[0])
        z = pair_ref[...].reshape(rows * total, chans).astype(F32)
        normed = (normalize(z, 1) * norm_ref[pl.ds(0, 1), :]).astype(BF16)
        normed_s[...] = normed.reshape(rows, total, chans)
        make_panels0()
    with mark("barrier"):
        pl.semaphore_wait(barrier, devices - 1)
    with mark("sendA"):
        push_all(mask_send, mask_recv.at[me], 0)
        push_near(lambda at: a_send.at[at], a_near.at[spot], 1)
        push_far(lambda at: a_send.at[at, 0], a_far.at[spot], 2, flip)
        mask_recv[me] = mask_send[...]
        a_near[spot] = a_send[spot]
    with mark("idleA"):
        gatew_s[...] = turn(gate_ref[0])
        outw_s[...] = turn(outw_ref[0])
        weight_s[1] = turn(proj_ref[1])
        for layer in range(2):
            mixg_s[layer] = jnp.broadcast_to(mix_ref[pl.ds(layer, 1), :], (total, hidden)).T
        normg_s[...] = jnp.broadcast_to(norm_ref[pl.ds(1, 1), :], (total, chans)).T
        rhs_s[...] = jnp.zeros(rhs_s.shape, BF16)
        zt_s[0] = turn(pair_ref[:, near_cols, :].reshape(spots, chans))
        make_gate0(0, normed_s[:, near_cols, :].reshape(spots, chans))
    with mark("waitmask"):
        wait_some(mask_recv, devices - 1, recv_sems.at[0])
    with mark("masks"):
        column_mask = jnp.sum(mask_recv[...], axis=0)
        doubled = jnp.where(lane // cols == half, column_mask, pltpu.roll(column_mask, cols, 1))
        set_scale(0, me, column_mask, doubled)
        set_scale(1, partner, column_mask, doubled)
    with mark("waitAnear"):
        wait_some(a_near, group - 1, recv_sems.at[1])
    with mark("out0"):
        right_s[...] = a_near[:, 1].astype(F32).reshape(group * rows * own, total)
        for c in range(own):
            right = (right_s[pl.ds(c, cols, stride=own), :] * column_mask).astype(BF16)
            rhs_s[c, 0:cols, 0:total] = right
            rhs_s[c, cols : 2 * cols, total : 2 * total] = right
        outgoing(0, a_near[:, 0])
    with mark("sendB0"):
        send_b(0)
        push(pair_ref.at[:, far_cols, :], pair_far, 3, partner)
    with mark("waitAfar"):
        wait_all(a_far, recv_sems.at[2])
    with mark("out1"):
        outgoing(1, a_far[...])
    with mark("sendB1"):
        send_b(1)
    with mark("waitB0"):
        wait_some(b_recv.at[0], group - 1, recv_sems.at[5])
    with mark("fin0"):
        finish0(0)
    with mark("sendC0"):
        send_c(0)
    with mark("waitpair"):
        wait_all(pair_far, recv_sems.at[3])
    with mark("pair"):
        z = pair_far[...].reshape(spots, chans)
        zt_s[1] = turn(z)
        make_gate0(1, (normalize(z.astype(F32), 1) * norm_ref[pl.ds(0, 1), :]).astype(BF16))
    with mark("waitB1"):
        wait_some(b_recv.at[1], group - 1, recv_sems.at[6])
    with mark("fin1"):
        finish0(1)
    with mark("sendC1"):
        send_c(1)
    with mark("nat0"):
        z1_s[0] = z1t_s[0].astype(F32).T.astype(BF16)
        natural(0, normed1_s[...].astype(F32).T.astype(BF16))
    with mark("waitC0"):
        wait_some(c_near.at[0], group - 1, recv_sems.at[7])
        wait_all(c_far.at[0], recv_sems.at[9])
    with mark("back"):
        push(z1t_s.at[1], back_recv, 4, partner)
    with mark("unpack0"):
        unpack1(0)
    with mark("waitC1"):
        wait_some(c_near.at[1], group - 1, recv_sems.at[8])
        wait_all(c_far.at[1], recv_sems.at[10])
    with mark("in"):
        unpack1(1)
        incoming()
    with mark("sendD"):
        push_near(lambda at: d_send.at[at], d_recv.at[spot], 11)
        d_recv[spot] = d_send[spot]
    with mark("waitback"):
        wait_all(back_recv, recv_sems.at[4])
    with mark("nat1"):
        z = back_recv[...].astype(F32).T
        z1_s[1] = z.astype(BF16)
        natural(1, (normalize(z, 1) * norm_ref[pl.ds(1, 1), :]).astype(BF16))
        wait_some(mask_recv, devices - 1, send_sems.at[0])
        wait_some(a_near, group - 1, send_sems.at[1])
        wait_all(a_far, send_sems.at[2])
        wait_all(pair_far, send_sems.at[3])
        wait_all(back_recv, send_sems.at[4])
        wait_all(c_far.at[0], send_sems.at[9])
        for part in range(2):
            wait_some(b_recv.at[part], group - 1, send_sems.at[5 + part])
            wait_some(c_near.at[part], group - 1, send_sems.at[7 + part])
        pass
        wait_all(c_far.at[1], send_sems.at[10])
    with mark("waitD"):
        wait_some(d_recv, group - 1, recv_sems.at[11])
    with mark("finish1"):
        finish1()
    wait_some(d_recv, group - 1, send_sems.at[11])


def fused(devices, pair, residue_mask, norm_gain, proj_weight, gate_weight, mix_gain, out_weight):
    rows, total, chans = pair.shape
    hidden = mix_gain.shape[1]
    group = devices // HALVES
    own = hidden // group
    cols = total // HALVES
    spots = rows * cols
    pairs = rows // 2
    half_rows = group * pairs * own
    hbm = pl.BlockSpec(memory_space=pltpu.HBM)
    params = (norm_gain, proj_weight, gate_weight, mix_gain, out_weight)
    operands = [
        pltpu.with_memory_space_constraint(v, pltpu.HBM) for v in (pair, residue_mask, *params)
    ]
    return pl.pallas_call(
        functools.partial(fused_kernel, devices),
        out_shape=pltpu.VMEM(pair.shape, BF16),
        in_specs=[hbm] * 7,
        out_specs=pl.BlockSpec(memory_space=pltpu.VMEM),
        scratch_shapes=[
            pltpu.VMEM(pair.shape, BF16),
            pltpu.SMEM(residue_mask.shape, jnp.int32),
            *(pltpu.VMEM(p.shape, p.dtype) for p in params),
            pltpu.VMEM((1, total), F32),
            pltpu.VMEM((devices, 1, total), F32),
            pltpu.VMEM((group, 2, rows * own, total), BF16),
            pltpu.VMEM((group, 2, rows * own, total), BF16),
            pltpu.VMEM((group, rows * own, total), BF16),
            pltpu.VMEM((rows, cols, chans), BF16),
            pltpu.VMEM((2, group, pairs * own, total), BF16),
            pltpu.VMEM((2, group, pairs * own, total), BF16),
            pltpu.VMEM((2, group, 2, pairs * own, total), BF16),
            pltpu.VMEM((2, group, 2, pairs * own, total), BF16),
            pltpu.VMEM((2, group, pairs * own, total), BF16),
            pltpu.VMEM((chans, spots), BF16),
            pltpu.VMEM((group, rows * own, total), BF16),
            pltpu.VMEM((group, rows * own, total), BF16),
            pltpu.VMEM((2, 4 * hidden, chans), BF16),
            pltpu.VMEM((chans, chans), BF16),
            pltpu.VMEM((chans, hidden), BF16),
            pltpu.VMEM((2, hidden, total), F32),
            pltpu.VMEM((chans, total), F32),
            pltpu.VMEM((2, 1, spots), F32),
            pltpu.VMEM((rows, total, chans), BF16),
            pltpu.VMEM((chans, spots), BF16),
            pltpu.VMEM((2, chans, spots), BF16),
            pltpu.VMEM((2, chans, spots), BF16),
            pltpu.VMEM((2, chans, spots), F32),
            pltpu.VMEM((2, spots, chans), BF16),
            pltpu.VMEM((2, spots, chans), F32),
            pltpu.VMEM((2, group * (rows * own + PAD), total), F32),
            pltpu.VMEM((group * rows * own, total), F32),
            pltpu.VMEM((own, total, 2 * total), BF16),
            pltpu.VMEM((2, half_rows, total), F32),
            pltpu.VMEM((2 * half_rows, total), F32),
            pltpu.VMEM((2 * half_rows, total), F32),
            pltpu.VMEM((2 * half_rows, total), F32),
            pltpu.VMEM((cols * own, total), F32),
            pltpu.SemaphoreType.DMA((12,)),
            pltpu.SemaphoreType.DMA((12,)),
            pltpu.SemaphoreType.DMA((7,)),
        ],
        compiler_params=pltpu.CompilerParams(
            collective_id=0, has_side_effects=True, vmem_limit_bytes=16777216
        ),
        name="triangles",
    )(*operands)


def panels(rows, mask_rows, mask_all, gain, weight):
    hidden = weight.shape[1] // 4
    mask_float = mask_all.astype(F32)
    normed = (normalize(rows.astype(F32), 2) * gain).astype(BF16)
    proj = jnp.einsum("rnc,ch->hrn", normed, weight, preferred_element_type=F32)
    scale = mask_rows.astype(F32)[:, None] * mask_float[None, :]
    left = (jax.nn.sigmoid(proj[:hidden]) * proj[hidden : 2 * hidden] * scale).astype(BF16)
    right = (jax.nn.sigmoid(proj[2 * hidden : 3 * hidden]) * proj[3 * hidden :] * scale).astype(
        BF16
    )
    return (normed, left, right)


def triangle(rows, mask_rows, mask_all, gain, weight, gate_w, tri_gain, out_w, second):
    normed, left, right = panels(rows, mask_rows, mask_all, gain, weight)
    left = lax.all_to_all(left, "dap", split_axis=0, concat_axis=1, tiled=True)
    right = lax.all_to_all(right, "dap", split_axis=0, concat_axis=1, tiled=True)
    spec = "cki,ckj->cij" if second else "cik,cjk->cij"
    tri = jnp.einsum(spec, left, right, preferred_element_type=F32).astype(BF16)
    tri = lax.all_to_all(tri, "dap", split_axis=1, concat_axis=0, tiled=True)
    gate = jax.nn.sigmoid(jnp.einsum("rnc,cd->rnd", normed, gate_w, preferred_element_type=F32))
    tri_normed = (normalize(tri.astype(F32), 0) * tri_gain[:, None, None]).astype(BF16)
    out = jnp.einsum("hrn,hc->rnc", tri_normed, out_w, preferred_element_type=F32)
    return (rows.astype(F32) + gate * out).astype(BF16)


def by_collectives(pair, residue_mask, *params):
    mask_all = lax.all_gather(residue_mask, "dap", axis=0, tiled=True)
    state = pair
    for layer in range(2):
        gain, weight, gate_w, tri_gain, out_w = (p[layer] for p in params)
        state = triangle(
            state, residue_mask, mask_all, gain, weight, gate_w, tri_gain, out_w, layer == 1
        )
    return state


def solution(mesh):
    devices = mesh.shape["dap"]

    def body(pair, residue_mask, norm_gain, proj_weight, gate_weight, mix_gain, out_weight):
        args = (pair, residue_mask, norm_gain, proj_weight, gate_weight, mix_gain, out_weight)
        group = devices // HALVES
        own = mix_gain.shape[1] // group
        rows, total, chans = pair.shape
        whole = group * HALVES == devices and group & (group - 1) == 0
        whole = whole and own * group == chans == mix_gain.shape[1] == total == 128
        if whole and own == 8 and rows == 4:
            return fused(devices, *args)
        return by_collectives(*args)

    return jax.shard_map(
        body,
        mesh=mesh,
        in_specs=(P("dap", None, None), P("dap"), P(), P(), P(), P(), P()),
        out_specs=P("dap", None, None),
        check_vma=False,
    )
```

```python
import contextlib
import functools

import jax
import jax.numpy as jnp
from jax import lax
from jax.experimental import pallas as pl
from jax.experimental.pallas import tpu as pltpu
from jax.sharding import PartitionSpec as P

EPS = 1e-05
F32 = jnp.float32
BF16 = jnp.bfloat16
MESH = pl.DeviceIdType.MESH
HALVES = 2
PAD = 8


def normalize(values, axis):
    center = values - jnp.mean(values, axis=axis, keepdims=True)
    spread = jnp.mean(center * center, axis=axis, keepdims=True)
    return center * lax.rsqrt(spread + EPS)


def normalize_down(values):
    moved = values - values[:1]
    center = jnp.mean(moved, axis=0, keepdims=True)
    spread = jnp.mean(moved * moved, axis=0, keepdims=True) - center * center
    return (moved - center) * lax.rsqrt(jnp.maximum(spread, 0.0) + EPS)


def dot(a, b, dims):
    return lax.dot_general(a, b, ((dims[:1], dims[1:]), ((), ())), preferred_element_type=F32)


def mark(name):
    return contextlib.nullcontext()


def fused_kernel(
    devices,
    pair_hbm,
    mask_hbm,
    norm_hbm,
    proj_hbm,
    gate_hbm,
    mix_hbm,
    outw_hbm,
    out_ref,
    pair_ref,
    mask_ref,
    norm_ref,
    proj_ref,
    gate_ref,
    mix_ref,
    outw_ref,
    mask_send,
    mask_recv,
    a_send,
    a_near,
    a_far,
    pair_far,
    b_send,
    b_recv,
    c_send,
    c_near,
    c_far,
    back_recv,
    d_send,
    d_recv,
    weight_s,
    gatew_s,
    outw_s,
    mixg_s,
    normg_s,
    scale_s,
    normed_s,
    normed1_s,
    zt_s,
    z1t_s,
    gate0_s,
    z1_s,
    gate1_s,
    left_s,
    right_s,
    rhs_s,
    flat_s,
    lhs1_s,
    own1_s,
    far1_s,
    flat1_s,
    send_sems,
    recv_sems,
    load_sems,
):
    rows, total, chans = pair_ref.shape
    hidden = mix_ref.shape[1]
    group = devices // HALVES
    own = hidden // group
    cols = total // HALVES
    spots = rows * cols
    pairs = rows // 2
    step = rows * own + PAD
    me = lax.axis_index("dap")
    half = me // group
    spot = lax.rem(me, group)
    partner = lax.rem(me + group, devices)
    zone = me * 4 // devices
    flip = jnp.where((zone == 0) | (zone == 3), group // 2, 0)
    near_cols = pl.ds(pl.multiple_of(half * cols, cols), cols)
    far_cols = pl.ds(pl.multiple_of((1 - half) * cols, cols), cols)

    barrier = pltpu.get_barrier_semaphore()

    def greet(step, carry):
        peer = me ^ (devices - step)
        pl.semaphore_signal(barrier, inc=1, device_id=(peer,), device_id_type=MESH)
        return carry

    lax.fori_loop(1, devices, greet, 0, unroll=True)

    sources = (pair_hbm, proj_hbm, mask_hbm, norm_hbm, gate_hbm, mix_hbm, outw_hbm)
    places = (pair_ref, proj_ref, mask_ref, norm_ref, gate_ref, mix_ref, outw_ref)
    loads = [
        pltpu.make_async_copy(source, place, load_sems.at[slot])
        for slot, (source, place) in enumerate(zip(sources, places))
    ]
    for load in loads:
        load.start()
    def push(src, dst, slot, peer):
        pltpu.make_async_remote_copy(
            src_ref=src,
            dst_ref=dst,
            send_sem=send_sems.at[slot],
            recv_sem=recv_sems.at[slot],
            device_id=(peer,),
            device_id_type=MESH,
        ).start()

    def push_near(src, dst, slot):
        for step in range(group // 2):
            high = group - 1 - step
            for bits in (high, high ^ (group // 2) ^ 1):
                if bits > 0:
                    push(src(spot ^ bits), dst, slot, me ^ bits)

    def push_far(src, dst, slot, turn_by=0):
        def one(step, carry):
            bits = (group - step) ^ turn_by
            push(src(spot ^ bits), dst, slot, me ^ (group + bits))
            return carry

        lax.fori_loop(1, group + 1, one, 0, unroll=True)

    def push_all(src, dst, slot):
        def one(step, carry):
            push(src, dst, slot, me ^ (devices - step))
            return carry

        lax.fori_loop(1, devices, one, 0, unroll=True)

    def wait_all(buf, sem):
        pltpu.make_async_copy(buf, buf, sem).wait()

    def wait_some(buf, count, sem):
        part = buf.at[pl.ds(0, count)]
        pltpu.make_async_copy(part, part, sem).wait()

    def lanes_of(parts):
        return jnp.concatenate(parts, axis=1)

    def panels_of(layer, normed, dims, side):
        at = 2 * side * hidden
        gate = dot(weight_s[layer, at : at + hidden], normed, dims)
        value = dot(weight_s[layer, at + hidden : at + 2 * hidden], normed, dims)
        return jax.nn.sigmoid(gate) * value

    def make_panels0():
        for pair in range(pairs):
            normed = normed_s[2 * pair : 2 * pair + 2].reshape(2 * total, chans)
            for side in range(2):
                panel = panels_of(0, normed, (1, 1), side)
                parts = [
                    (panel[:, r * total : (r + 1) * total] * mask_ref[2 * pair + r].astype(F32))
                    for r in range(2)
                ]
                tile = jnp.concatenate([p.reshape(group, own, total) for p in parts], axis=1)
                at = pl.ds(2 * own * pair, 2 * own)
                a_send[:, side, at, :] = tile.astype(BF16)

    def make_gate0(part, normed):
        gate0_s[part] = jax.nn.sigmoid(dot(gatew_s[...], normed, (1, 1)))

    def turn(values):
        return values.astype(F32).T.astype(BF16)

    def set_scale(part, owner, column_mask, doubled):
        entry = [
            jnp.sum(jnp.where(lane == owner * rows + r, column_mask, 0.0), axis=1, keepdims=True)
            for r in range(rows)
        ]
        scale_s[part] = lanes_of(
            [
                jnp.where(lane < cols, entry[2 * p], entry[2 * p + 1]) * doubled
                for p in range(pairs)
            ]
        )

    def outgoing(part, panel):
        for p in range(group):
            left_s[part, p * step : p * step + rows * own, :] = panel[p].astype(F32)
        for c in range(own):
            left = jnp.concatenate(
                [
                    lanes_of(
                        [
                            left_s[part, pl.ds((2 * p + r) * own + c, group, stride=step), :]
                            for r in range(2)
                        ]
                    )
                    for p in range(pairs)
                ],
                axis=0,
            ).astype(BF16)
            tri = dot(left, rhs_s[c], (1, 1))
            for p in range(pairs):
                flat_s[part, pl.ds(p * own + c, group, stride=pairs * own), :] = tri[
                    p * group : (p + 1) * group
                ]
        b_send[part] = flat_s[part].reshape(group, pairs * own, total).astype(BF16)

    def send_b(part):
        push_near(lambda at: b_send.at[part, at], b_recv.at[part, spot], 5 + part)
        b_recv[part, spot] = b_send[part, spot]

    def finish0(part):
        got = b_recv[part].astype(F32)
        tri = lanes_of(
            [got[:, p * own : (p + 1) * own].reshape(hidden, total) for p in range(pairs)]
        )
        gain = mixg_s[0]
        tri_normed = (normalize_down(tri) * lanes_of([gain] * pairs)).astype(BF16)
        out = lanes_of(
            [
                dot(outw_s[...], tri_normed[:, p * total : (p + 1) * total], (1, 0))
                for p in range(pairs)
            ]
        )
        new = (zt_s[part].astype(F32) + gate0_s[part] * out).astype(BF16)
        z1t_s[part] = new
        normed = (normalize_down(new.astype(F32)) * lanes_of([normg_s[...]] * pairs)).astype(BF16)
        if part == 0:
            normed1_s[...] = normed
        for side in (1, 0):
            panel = panels_of(1, normed, (1, 0), side) * scale_s[part]
            tile = jnp.concatenate(
                [
                    panel[:, p * total : (p + 1) * total].reshape(group, own, total)
                    for p in range(pairs)
                ],
                axis=1,
            )
            c_send[part, :, side] = tile.astype(BF16)
            if side == 1:
                push_far(
                    lambda at: c_send.at[part, at, 1], c_far.at[part, spot], 9 + part, flip
                )

    def send_c(part):
        push_near(lambda at: c_send.at[part, at], c_near.at[part, spot], 7 + part)
        c_near[part, spot] = c_send[part, spot]

    def natural(part, normed):
        gate1_s[part] = jax.nn.sigmoid(dot(normed, gate_ref[1], (1, 0)))

    def unpack1(part):
        size = group * pairs * own
        at = pl.ds(part * size, size)
        near = c_near[part].astype(F32)
        lhs1_s[at, :] = near[:, 0].reshape(size, total)
        own1_s[at, :] = near[:, 1].reshape(size, total)
        far1_s[pl.ds((1 - part) * size, size), :] = c_far[part].astype(F32).reshape(size, total)

    def incoming():
        count = HALVES * group * pairs
        low = lane < cols
        for c in range(own):
            pick = pl.ds(c, count, stride=own)
            left = lhs1_s[pick, :].astype(BF16).T
            right = lanes_of([own1_s[pick, :], far1_s[pick, :]]).astype(BF16)
            prod = dot(left, right, (1, 0))
            straight = jnp.where(low, prod[:cols, :total], prod[cols:, total:])
            crossed = jnp.where(low, prod[:cols, total:], prod[cols:, :total])
            tri = straight + pltpu.roll(crossed, cols, 1)
            flat1_s[pl.ds(c, cols, stride=own), :] = tri
        d_send[...] = flat1_s[...].reshape(group, rows * own, total).astype(BF16)

    def finish1():
        got = d_recv[...].astype(F32)
        for r in range(rows):
            tri = got[:, r * own : (r + 1) * own].reshape(hidden, total)
            tri_normed = (normalize_down(tri) * mixg_s[1]).astype(BF16)
            out = dot(tri_normed, outw_ref[1], (0, 0))
            block = pl.ds(r * cols, cols)
            for part, place in enumerate((near_cols, far_cols)):
                piece = out[part * cols : (part + 1) * cols]
                new = z1_s[part, block, :].astype(F32) + gate1_s[part, block, :] * piece
                out_ref[r, place, :] = new.astype(BF16)

    lane = lax.broadcasted_iota(jnp.int32, (1, total), 1)
    with mark("load"):
        for load in loads:
            load.wait()
    with mark("panels0"):
        mask_row = jnp.zeros((1, total), F32)
        for r in range(rows):
            mask_row = mask_row + jnp.where(lane == me * rows + r, mask_ref[r].astype(F32), 0.0)
        mask_send[...] = mask_row
        weight_s[0] = turn(proj_ref[0])
        z = pair_ref[...].reshape(rows * total, chans).astype(F32)
        normed = (normalize(z, 1) * norm_ref[pl.ds(0, 1), :]).astype(BF16)
        normed_s[...] = normed.reshape(rows, total, chans)
        make_panels0()
    with mark("barrier"):
        pl.semaphore_wait(barrier, devices - 1)
    with mark("sendA"):
        push_all(mask_send, mask_recv.at[me], 0)
        push_near(lambda at: a_send.at[at], a_near.at[spot], 1)
        push_far(lambda at: a_send.at[at, 0], a_far.at[spot], 2, flip)
        mask_recv[me] = mask_send[...]
        a_near[spot] = a_send[spot]
    with mark("idleA"):
        gatew_s[...] = turn(gate_ref[0])
        outw_s[...] = turn(outw_ref[0])
        weight_s[1] = turn(proj_ref[1])
        for layer in range(2):
            mixg_s[layer] = jnp.broadcast_to(mix_ref[pl.ds(layer, 1), :], (total, hidden)).T
        normg_s[...] = jnp.broadcast_to(norm_ref[pl.ds(1, 1), :], (total, chans)).T
        rhs_s[...] = jnp.zeros(rhs_s.shape, BF16)
        zt_s[0] = turn(pair_ref[:, near_cols, :].reshape(spots, chans))
        make_gate0(0, normed_s[:, near_cols, :].reshape(spots, chans))
    with mark("waitmask"):
        wait_some(mask_recv, devices - 1, recv_sems.at[0])
    with mark("masks"):
        column_mask = jnp.sum(mask_recv[...], axis=0)
        doubled = jnp.where(lane // cols == half, column_mask, pltpu.roll(column_mask, cols, 1))
        set_scale(0, me, column_mask, doubled)
        set_scale(1, partner, column_mask, doubled)
    with mark("waitAnear"):
        wait_some(a_near, group - 1, recv_sems.at[1])
    with mark("out0"):
        right_s[...] = a_near[:, 1].astype(F32).reshape(group * rows * own, total)
        for c in range(own):
            right = (right_s[pl.ds(c, cols, stride=own), :] * column_mask).astype(BF16)
            rhs_s[c, 0:cols, 0:total] = right
            rhs_s[c, cols : 2 * cols, total : 2 * total] = right
        outgoing(0, a_near[:, 0])
    with mark("sendB0"):
        send_b(0)
        push(pair_ref.at[:, far_cols, :], pair_far, 3, partner)
    with mark("waitAfar"):
        wait_all(a_far, recv_sems.at[2])
    with mark("out1"):
        outgoing(1, a_far[...])
    with mark("sendB1"):
        send_b(1)
    with mark("waitB0"):
        wait_some(b_recv.at[0], group - 1, recv_sems.at[5])
    with mark("fin0"):
        finish0(0)
    with mark("sendC0"):
        send_c(0)
    with mark("waitpair"):
        wait_all(pair_far, recv_sems.at[3])
    with mark("pair"):
        z = pair_far[...].reshape(spots, chans)
        zt_s[1] = turn(z)
        make_gate0(1, (normalize(z.astype(F32), 1) * norm_ref[pl.ds(0, 1), :]).astype(BF16))
    with mark("waitB1"):
        wait_some(b_recv.at[1], group - 1, recv_sems.at[6])
    with mark("fin1"):
        finish0(1)
    with mark("sendC1"):
        send_c(1)
    with mark("nat0"):
        z1_s[0] = z1t_s[0].astype(F32).T.astype(BF16)
        natural(0, normed1_s[...].astype(F32).T.astype(BF16))
    with mark("waitC0"):
        wait_some(c_near.at[0], group - 1, recv_sems.at[7])
        wait_all(c_far.at[0], recv_sems.at[9])
    with mark("back"):
        push(z1t_s.at[1], back_recv, 4, partner)
    with mark("unpack0"):
        unpack1(0)
    with mark("waitC1"):
        wait_some(c_near.at[1], group - 1, recv_sems.at[8])
        wait_all(c_far.at[1], recv_sems.at[10])
    with mark("in"):
        unpack1(1)
        incoming()
    with mark("sendD"):
        push_near(lambda at: d_send.at[at], d_recv.at[spot], 11)
        d_recv[spot] = d_send[spot]
    with mark("waitback"):
        wait_all(back_recv, recv_sems.at[4])
    with mark("nat1"):
        z = back_recv[...].astype(F32).T
        z1_s[1] = z.astype(BF16)
        natural(1, (normalize(z, 1) * norm_ref[pl.ds(1, 1), :]).astype(BF16))
        wait_some(mask_recv, devices - 1, send_sems.at[0])
        wait_some(a_near, group - 1, send_sems.at[1])
        wait_all(a_far, send_sems.at[2])
        wait_all(pair_far, send_sems.at[3])
        wait_all(back_recv, send_sems.at[4])
        wait_all(c_far.at[0], send_sems.at[9])
        for part in range(2):
            wait_some(b_recv.at[part], group - 1, send_sems.at[5 + part])
            wait_some(c_near.at[part], group - 1, send_sems.at[7 + part])
        pass
        wait_all(c_far.at[1], send_sems.at[10])
    with mark("waitD"):
        wait_some(d_recv, group - 1, recv_sems.at[11])
    with mark("finish1"):
        finish1()
    wait_some(d_recv, group - 1, send_sems.at[11])


def fused(devices, pair, residue_mask, norm_gain, proj_weight, gate_weight, mix_gain, out_weight):
    rows, total, chans = pair.shape
    hidden = mix_gain.shape[1]
    group = devices // HALVES
    own = hidden // group
    cols = total // HALVES
    spots = rows * cols
    pairs = rows // 2
    half_rows = group * pairs * own
    hbm = pl.BlockSpec(memory_space=pltpu.HBM)
    params = (norm_gain, proj_weight, gate_weight, mix_gain, out_weight)
    operands = [
        pltpu.with_memory_space_constraint(v, pltpu.HBM) for v in (pair, residue_mask, *params)
    ]
    return pl.pallas_call(
        functools.partial(fused_kernel, devices),
        out_shape=pltpu.VMEM(pair.shape, BF16),
        in_specs=[hbm] * 7,
        out_specs=pl.BlockSpec(memory_space=pltpu.VMEM),
        scratch_shapes=[
            pltpu.VMEM(pair.shape, BF16),
            pltpu.SMEM(residue_mask.shape, jnp.int32),
            *(pltpu.VMEM(p.shape, p.dtype) for p in params),
            pltpu.VMEM((1, total), F32),
            pltpu.VMEM((devices, 1, total), F32),
            pltpu.VMEM((group, 2, rows * own, total), BF16),
            pltpu.VMEM((group, 2, rows * own, total), BF16),
            pltpu.VMEM((group, rows * own, total), BF16),
            pltpu.VMEM((rows, cols, chans), BF16),
            pltpu.VMEM((2, group, pairs * own, total), BF16),
            pltpu.VMEM((2, group, pairs * own, total), BF16),
            pltpu.VMEM((2, group, 2, pairs * own, total), BF16),
            pltpu.VMEM((2, group, 2, pairs * own, total), BF16),
            pltpu.VMEM((2, group, pairs * own, total), BF16),
            pltpu.VMEM((chans, spots), BF16),
            pltpu.VMEM((group, rows * own, total), BF16),
            pltpu.VMEM((group, rows * own, total), BF16),
            pltpu.VMEM((2, 4 * hidden, chans), BF16),
            pltpu.VMEM((chans, chans), BF16),
            pltpu.VMEM((chans, hidden), BF16),
            pltpu.VMEM((2, hidden, total), F32),
            pltpu.VMEM((chans, total), F32),
            pltpu.VMEM((2, 1, spots), F32),
            pltpu.VMEM((rows, total, chans), BF16),
            pltpu.VMEM((chans, spots), BF16),
            pltpu.VMEM((2, chans, spots), BF16),
            pltpu.VMEM((2, chans, spots), BF16),
            pltpu.VMEM((2, chans, spots), F32),
            pltpu.VMEM((2, spots, chans), BF16),
            pltpu.VMEM((2, spots, chans), F32),
            pltpu.VMEM((2, group * (rows * own + PAD), total), F32),
            pltpu.VMEM((group * rows * own, total), F32),
            pltpu.VMEM((own, total, 2 * total), BF16),
            pltpu.VMEM((2, half_rows, total), F32),
            pltpu.VMEM((2 * half_rows, total), F32),
            pltpu.VMEM((2 * half_rows, total), F32),
            pltpu.VMEM((2 * half_rows, total), F32),
            pltpu.VMEM((cols * own, total), F32),
            pltpu.SemaphoreType.DMA((12,)),
            pltpu.SemaphoreType.DMA((12,)),
            pltpu.SemaphoreType.DMA((7,)),
        ],
        compiler_params=pltpu.CompilerParams(
            collective_id=0, has_side_effects=True, vmem_limit_bytes=16777216
        ),
        name="triangles",
    )(*operands)


def panels(rows, mask_rows, mask_all, gain, weight):
    hidden = weight.shape[1] // 4
    mask_float = mask_all.astype(F32)
    normed = (normalize(rows.astype(F32), 2) * gain).astype(BF16)
    proj = jnp.einsum("rnc,ch->hrn", normed, weight, preferred_element_type=F32)
    scale = mask_rows.astype(F32)[:, None] * mask_float[None, :]
    left = (jax.nn.sigmoid(proj[:hidden]) * proj[hidden : 2 * hidden] * scale).astype(BF16)
    right = (jax.nn.sigmoid(proj[2 * hidden : 3 * hidden]) * proj[3 * hidden :] * scale).astype(
        BF16
    )
    return (normed, left, right)


def triangle(rows, mask_rows, mask_all, gain, weight, gate_w, tri_gain, out_w, second):
    normed, left, right = panels(rows, mask_rows, mask_all, gain, weight)
    left = lax.all_to_all(left, "dap", split_axis=0, concat_axis=1, tiled=True)
    right = lax.all_to_all(right, "dap", split_axis=0, concat_axis=1, tiled=True)
    spec = "cki,ckj->cij" if second else "cik,cjk->cij"
    tri = jnp.einsum(spec, left, right, preferred_element_type=F32).astype(BF16)
    tri = lax.all_to_all(tri, "dap", split_axis=1, concat_axis=0, tiled=True)
    gate = jax.nn.sigmoid(jnp.einsum("rnc,cd->rnd", normed, gate_w, preferred_element_type=F32))
    tri_normed = (normalize(tri.astype(F32), 0) * tri_gain[:, None, None]).astype(BF16)
    out = jnp.einsum("hrn,hc->rnc", tri_normed, out_w, preferred_element_type=F32)
    return (rows.astype(F32) + gate * out).astype(BF16)


def by_collectives(pair, residue_mask, *params):
    mask_all = lax.all_gather(residue_mask, "dap", axis=0, tiled=True)
    state = pair
    for layer in range(2):
        gain, weight, gate_w, tri_gain, out_w = (p[layer] for p in params)
        state = triangle(
            state, residue_mask, mask_all, gain, weight, gate_w, tri_gain, out_w, layer == 1
        )
    return state


def solution(mesh):
    devices = mesh.shape["dap"]

    def body(pair, residue_mask, norm_gain, proj_weight, gate_weight, mix_gain, out_weight):
        args = (pair, residue_mask, norm_gain, proj_weight, gate_weight, mix_gain, out_weight)
        group = devices // HALVES
        own = mix_gain.shape[1] // group
        rows, total, chans = pair.shape
        whole = group * HALVES == devices and group & (group - 1) == 0
        whole = whole and own * group == chans == mix_gain.shape[1] == total == 128
        if whole and own == 8 and rows == 4:
            return fused(devices, *args)
        return by_collectives(*args)

    return jax.shard_map(
        body,
        mesh=mesh,
        in_specs=(P("dap", None, None), P("dap"), P(), P(), P(), P(), P()),
        out_specs=P("dap", None, None),
        check_vma=False,
    )
```

```python
import contextlib
import functools

import jax
import jax.numpy as jnp
from jax import lax
from jax.experimental import pallas as pl
from jax.experimental.pallas import tpu as pltpu
from jax.sharding import PartitionSpec as P

EPS = 1e-05
F32 = jnp.float32
BF16 = jnp.bfloat16
MESH = pl.DeviceIdType.MESH
HALVES = 2
PAD = 8


def normalize(values, axis):
    center = values - jnp.mean(values, axis=axis, keepdims=True)
    spread = jnp.mean(center * center, axis=axis, keepdims=True)
    return center * lax.rsqrt(spread + EPS)


def normalize_down(values):
    moved = values - values[:1]
    center = jnp.mean(moved, axis=0, keepdims=True)
    spread = jnp.mean(moved * moved, axis=0, keepdims=True) - center * center
    return (moved - center) * lax.rsqrt(jnp.maximum(spread, 0.0) + EPS)


def dot(a, b, dims):
    return lax.dot_general(a, b, ((dims[:1], dims[1:]), ((), ())), preferred_element_type=F32)


def mark(name):
    return contextlib.nullcontext()


def fused_kernel(
    devices,
    pair_hbm,
    mask_hbm,
    norm_hbm,
    proj_hbm,
    gate_hbm,
    mix_hbm,
    outw_hbm,
    out_ref,
    pair_ref,
    mask_ref,
    norm_ref,
    proj_ref,
    gate_ref,
    mix_ref,
    outw_ref,
    mask_send,
    mask_recv,
    a_send,
    a_near,
    a_far,
    pair_far,
    b_send,
    b_recv,
    c_send,
    c_near,
    c_far,
    back_recv,
    d_send,
    d_recv,
    weight_s,
    gatew_s,
    outw_s,
    mixg_s,
    normg_s,
    scale_s,
    normed_s,
    normed1_s,
    zt_s,
    z1t_s,
    gate0_s,
    z1_s,
    gate1_s,
    left_s,
    right_s,
    rhs_s,
    flat_s,
    lhs1_s,
    own1_s,
    far1_s,
    flat1_s,
    send_sems,
    recv_sems,
    load_sems,
):
    rows, total, chans = pair_ref.shape
    hidden = mix_ref.shape[1]
    group = devices // HALVES
    own = hidden // group
    cols = total // HALVES
    spots = rows * cols
    pairs = rows // 2
    step = rows * own + PAD
    me = lax.axis_index("dap")
    half = me // group
    spot = lax.rem(me, group)
    partner = lax.rem(me + group, devices)
    zone = me * 4 // devices
    flip = jnp.where((zone == 0) | (zone == 3), group // 2, 0)
    near_cols = pl.ds(pl.multiple_of(half * cols, cols), cols)
    far_cols = pl.ds(pl.multiple_of((1 - half) * cols, cols), cols)

    barrier = pltpu.get_barrier_semaphore()

    def greet(step, carry):
        peer = me ^ (devices - step)
        pl.semaphore_signal(barrier, inc=1, device_id=(peer,), device_id_type=MESH)
        return carry

    lax.fori_loop(1, devices, greet, 0, unroll=True)

    sources = (pair_hbm, proj_hbm, mask_hbm, norm_hbm, gate_hbm, mix_hbm, outw_hbm)
    places = (pair_ref, proj_ref, mask_ref, norm_ref, gate_ref, mix_ref, outw_ref)
    loads = [
        pltpu.make_async_copy(source, place, load_sems.at[slot])
        for slot, (source, place) in enumerate(zip(sources, places))
    ]
    for load in loads:
        load.start()
    def push(src, dst, slot, peer):
        pltpu.make_async_remote_copy(
            src_ref=src,
            dst_ref=dst,
            send_sem=send_sems.at[slot],
            recv_sem=recv_sems.at[slot],
            device_id=(peer,),
            device_id_type=MESH,
        ).start()

    def push_near(src, dst, slot):
        for step in range(group // 2):
            high = group - 1 - step
            for bits in (high, high ^ (group // 2) ^ 1):
                if bits > 0:
                    push(src(spot ^ bits), dst, slot, me ^ bits)

    def push_far(src, dst, slot, turn_by=0):
        def one(step, carry):
            bits = (group - step) ^ turn_by
            push(src(spot ^ bits), dst, slot, me ^ (group + bits))
            return carry

        lax.fori_loop(1, group + 1, one, 0, unroll=True)

    def push_all(src, dst, slot):
        def one(step, carry):
            push(src, dst, slot, me ^ (devices - step))
            return carry

        lax.fori_loop(1, devices, one, 0, unroll=True)

    def wait_all(buf, sem):
        pltpu.make_async_copy(buf, buf, sem).wait()

    def wait_some(buf, count, sem):
        part = buf.at[pl.ds(0, count)]
        pltpu.make_async_copy(part, part, sem).wait()

    def lanes_of(parts):
        return jnp.concatenate(parts, axis=1)

    def panels_of(layer, normed, dims, side):
        at = 2 * side * hidden
        gate = dot(weight_s[layer, at : at + hidden], normed, dims)
        value = dot(weight_s[layer, at + hidden : at + 2 * hidden], normed, dims)
        return jax.nn.sigmoid(gate) * value

    def make_panels0():
        for pair in range(pairs):
            normed = normed_s[2 * pair : 2 * pair + 2].reshape(2 * total, chans)
            for side in range(2):
                panel = panels_of(0, normed, (1, 1), side)
                parts = [
                    (panel[:, r * total : (r + 1) * total] * mask_ref[2 * pair + r].astype(F32))
                    for r in range(2)
                ]
                tile = jnp.concatenate([p.reshape(group, own, total) for p in parts], axis=1)
                at = pl.ds(2 * own * pair, 2 * own)
                a_send[:, side, at, :] = tile.astype(BF16)

    def make_gate0(part, normed):
        gate0_s[part] = jax.nn.sigmoid(dot(gatew_s[...], normed, (1, 1)))

    def turn(values):
        return values.astype(F32).T.astype(BF16)

    def set_scale(part, owner, column_mask, doubled):
        entry = [
            jnp.sum(jnp.where(lane == owner * rows + r, column_mask, 0.0), axis=1, keepdims=True)
            for r in range(rows)
        ]
        scale_s[part] = lanes_of(
            [
                jnp.where(lane < cols, entry[2 * p], entry[2 * p + 1]) * doubled
                for p in range(pairs)
            ]
        )

    def outgoing(part, panel):
        for p in range(group):
            left_s[part, p * step : p * step + rows * own, :] = panel[p].astype(F32)
        for c in range(own):
            left = jnp.concatenate(
                [
                    lanes_of(
                        [
                            left_s[part, pl.ds((2 * p + r) * own + c, group, stride=step), :]
                            for r in range(2)
                        ]
                    )
                    for p in range(pairs)
                ],
                axis=0,
            ).astype(BF16)
            tri = dot(left, rhs_s[c], (1, 1))
            for p in range(pairs):
                flat_s[part, pl.ds(p * own + c, group, stride=pairs * own), :] = tri[
                    p * group : (p + 1) * group
                ]
        b_send[part] = flat_s[part].reshape(group, pairs * own, total).astype(BF16)

    def send_b(part):
        push_near(lambda at: b_send.at[part, at], b_recv.at[part, spot], 5 + part)
        b_recv[part, spot] = b_send[part, spot]

    def finish0(part):
        got = b_recv[part].astype(F32)
        tri = lanes_of(
            [got[:, p * own : (p + 1) * own].reshape(hidden, total) for p in range(pairs)]
        )
        gain = mixg_s[0]
        tri_normed = (normalize_down(tri) * lanes_of([gain] * pairs)).astype(BF16)
        out = lanes_of(
            [
                dot(outw_s[...], tri_normed[:, p * total : (p + 1) * total], (1, 0))
                for p in range(pairs)
            ]
        )
        new = (zt_s[part].astype(F32) + gate0_s[part] * out).astype(BF16)
        z1t_s[part] = new
        normed = (normalize_down(new.astype(F32)) * lanes_of([normg_s[...]] * pairs)).astype(BF16)
        if part == 0:
            normed1_s[...] = normed
        for side in (1, 0):
            panel = panels_of(1, normed, (1, 0), side) * scale_s[part]
            tile = jnp.concatenate(
                [
                    panel[:, p * total : (p + 1) * total].reshape(group, own, total)
                    for p in range(pairs)
                ],
                axis=1,
            )
            c_send[part, :, side] = tile.astype(BF16)
            if side == 1:
                push_far(
                    lambda at: c_send.at[part, at, 1], c_far.at[part, spot], 9 + part, flip
                )

    def send_c(part):
        push_near(lambda at: c_send.at[part, at], c_near.at[part, spot], 7 + part)
        c_near[part, spot] = c_send[part, spot]

    def natural(part, normed):
        gate1_s[part] = jax.nn.sigmoid(dot(normed, gate_ref[1], (1, 0)))

    def unpack1(part):
        size = group * pairs * own
        at = pl.ds(part * size, size)
        near = c_near[part].astype(F32)
        lhs1_s[at, :] = near[:, 0].reshape(size, total)
        own1_s[at, :] = near[:, 1].reshape(size, total)
        far1_s[pl.ds((1 - part) * size, size), :] = c_far[part].astype(F32).reshape(size, total)

    def incoming():
        count = HALVES * group * pairs
        low = lane < cols
        for c in range(own):
            pick = pl.ds(c, count, stride=own)
            left = lhs1_s[pick, :].astype(BF16).T
            right = lanes_of([own1_s[pick, :], far1_s[pick, :]]).astype(BF16)
            prod = dot(left, right, (1, 0))
            straight = jnp.where(low, prod[:cols, :total], prod[cols:, total:])
            crossed = jnp.where(low, prod[:cols, total:], prod[cols:, :total])
            tri = straight + pltpu.roll(crossed, cols, 1)
            flat1_s[pl.ds(c, cols, stride=own), :] = tri
        d_send[...] = flat1_s[...].reshape(group, rows * own, total).astype(BF16)

    def finish1():
        got = d_recv[...].astype(F32)
        for r in range(rows):
            tri = got[:, r * own : (r + 1) * own].reshape(hidden, total)
            tri_normed = (normalize_down(tri) * mixg_s[1]).astype(BF16)
            out = dot(tri_normed, outw_ref[1], (0, 0))
            block = pl.ds(r * cols, cols)
            for part, place in enumerate((near_cols, far_cols)):
                piece = out[part * cols : (part + 1) * cols]
                new = z1_s[part, block, :].astype(F32) + gate1_s[part, block, :] * piece
                out_ref[r, place, :] = new.astype(BF16)

    lane = lax.broadcasted_iota(jnp.int32, (1, total), 1)
    with mark("load"):
        for load in loads[:4]:
            load.wait()
    with mark("panels0"):
        mask_row = jnp.zeros((1, total), F32)
        for r in range(rows):
            mask_row = mask_row + jnp.where(lane == me * rows + r, mask_ref[r].astype(F32), 0.0)
        mask_send[...] = mask_row
        weight_s[0] = turn(proj_ref[0])
        z = pair_ref[...].reshape(rows * total, chans).astype(F32)
        normed = (normalize(z, 1) * norm_ref[pl.ds(0, 1), :]).astype(BF16)
        normed_s[...] = normed.reshape(rows, total, chans)
        make_panels0()
    with mark("barrier"):
        pl.semaphore_wait(barrier, devices - 1)
    with mark("sendA"):
        push_all(mask_send, mask_recv.at[me], 0)
        push_near(lambda at: a_send.at[at], a_near.at[spot], 1)
        push_far(lambda at: a_send.at[at, 0], a_far.at[spot], 2, flip)
        mask_recv[me] = mask_send[...]
        a_near[spot] = a_send[spot]
    with mark("idleA"):
        for load in loads[4:]:
            load.wait()
        gatew_s[...] = turn(gate_ref[0])
        outw_s[...] = turn(outw_ref[0])
        weight_s[1] = turn(proj_ref[1])
        for layer in range(2):
            mixg_s[layer] = jnp.broadcast_to(mix_ref[pl.ds(layer, 1), :], (total, hidden)).T
        normg_s[...] = jnp.broadcast_to(norm_ref[pl.ds(1, 1), :], (total, chans)).T
        rhs_s[...] = jnp.zeros(rhs_s.shape, BF16)
        zt_s[0] = turn(pair_ref[:, near_cols, :].reshape(spots, chans))
        make_gate0(0, normed_s[:, near_cols, :].reshape(spots, chans))
    with mark("waitmask"):
        wait_some(mask_recv, devices - 1, recv_sems.at[0])
    with mark("masks"):
        column_mask = jnp.sum(mask_recv[...], axis=0)
        doubled = jnp.where(lane // cols == half, column_mask, pltpu.roll(column_mask, cols, 1))
        set_scale(0, me, column_mask, doubled)
        set_scale(1, partner, column_mask, doubled)
    with mark("waitAnear"):
        wait_some(a_near, group - 1, recv_sems.at[1])
    with mark("out0"):
        right_s[...] = a_near[:, 1].astype(F32).reshape(group * rows * own, total)
        for c in range(own):
            right = (right_s[pl.ds(c, cols, stride=own), :] * column_mask).astype(BF16)
            rhs_s[c, 0:cols, 0:total] = right
            rhs_s[c, cols : 2 * cols, total : 2 * total] = right
        outgoing(0, a_near[:, 0])
    with mark("sendB0"):
        send_b(0)
        push(pair_ref.at[:, far_cols, :], pair_far, 3, partner)
    with mark("waitAfar"):
        wait_all(a_far, recv_sems.at[2])
    with mark("out1"):
        outgoing(1, a_far[...])
    with mark("sendB1"):
        send_b(1)
    with mark("waitB0"):
        wait_some(b_recv.at[0], group - 1, recv_sems.at[5])
    with mark("fin0"):
        finish0(0)
    with mark("sendC0"):
        send_c(0)
    with mark("waitpair"):
        wait_all(pair_far, recv_sems.at[3])
    with mark("pair"):
        z = pair_far[...].reshape(spots, chans)
        zt_s[1] = turn(z)
        make_gate0(1, (normalize(z.astype(F32), 1) * norm_ref[pl.ds(0, 1), :]).astype(BF16))
    with mark("waitB1"):
        wait_some(b_recv.at[1], group - 1, recv_sems.at[6])
    with mark("fin1"):
        finish0(1)
    with mark("sendC1"):
        send_c(1)
    with mark("nat0"):
        z1_s[0] = z1t_s[0].astype(F32).T.astype(BF16)
        natural(0, normed1_s[...].astype(F32).T.astype(BF16))
    with mark("waitC0"):
        wait_some(c_near.at[0], group - 1, recv_sems.at[7])
        wait_all(c_far.at[0], recv_sems.at[9])
    with mark("back"):
        push(z1t_s.at[1], back_recv, 4, partner)
    with mark("unpack0"):
        unpack1(0)
    with mark("waitC1"):
        wait_some(c_near.at[1], group - 1, recv_sems.at[8])
        wait_all(c_far.at[1], recv_sems.at[10])
    with mark("in"):
        unpack1(1)
        incoming()
    with mark("sendD"):
        push_near(lambda at: d_send.at[at], d_recv.at[spot], 11)
        d_recv[spot] = d_send[spot]
    with mark("waitback"):
        wait_all(back_recv, recv_sems.at[4])
    with mark("nat1"):
        z = back_recv[...].astype(F32).T
        z1_s[1] = z.astype(BF16)
        natural(1, (normalize(z, 1) * norm_ref[pl.ds(1, 1), :]).astype(BF16))
        wait_some(mask_recv, devices - 1, send_sems.at[0])
        wait_some(a_near, group - 1, send_sems.at[1])
        wait_all(a_far, send_sems.at[2])
        wait_all(pair_far, send_sems.at[3])
        wait_all(back_recv, send_sems.at[4])
        wait_all(c_far.at[0], send_sems.at[9])
        for part in range(2):
            wait_some(b_recv.at[part], group - 1, send_sems.at[5 + part])
            wait_some(c_near.at[part], group - 1, send_sems.at[7 + part])
        pass
        wait_all(c_far.at[1], send_sems.at[10])
    with mark("waitD"):
        wait_some(d_recv, group - 1, recv_sems.at[11])
    with mark("finish1"):
        finish1()
    wait_some(d_recv, group - 1, send_sems.at[11])


def fused(devices, pair, residue_mask, norm_gain, proj_weight, gate_weight, mix_gain, out_weight):
    rows, total, chans = pair.shape
    hidden = mix_gain.shape[1]
    group = devices // HALVES
    own = hidden // group
    cols = total // HALVES
    spots = rows * cols
    pairs = rows // 2
    half_rows = group * pairs * own
    hbm = pl.BlockSpec(memory_space=pltpu.HBM)
    params = (norm_gain, proj_weight, gate_weight, mix_gain, out_weight)
    operands = [
        pltpu.with_memory_space_constraint(v, pltpu.HBM) for v in (pair, residue_mask, *params)
    ]
    return pl.pallas_call(
        functools.partial(fused_kernel, devices),
        out_shape=pltpu.VMEM(pair.shape, BF16),
        in_specs=[hbm] * 7,
        out_specs=pl.BlockSpec(memory_space=pltpu.VMEM),
        scratch_shapes=[
            pltpu.VMEM(pair.shape, BF16),
            pltpu.SMEM(residue_mask.shape, jnp.int32),
            *(pltpu.VMEM(p.shape, p.dtype) for p in params),
            pltpu.VMEM((1, total), F32),
            pltpu.VMEM((devices, 1, total), F32),
            pltpu.VMEM((group, 2, rows * own, total), BF16),
            pltpu.VMEM((group, 2, rows * own, total), BF16),
            pltpu.VMEM((group, rows * own, total), BF16),
            pltpu.VMEM((rows, cols, chans), BF16),
            pltpu.VMEM((2, group, pairs * own, total), BF16),
            pltpu.VMEM((2, group, pairs * own, total), BF16),
            pltpu.VMEM((2, group, 2, pairs * own, total), BF16),
            pltpu.VMEM((2, group, 2, pairs * own, total), BF16),
            pltpu.VMEM((2, group, pairs * own, total), BF16),
            pltpu.VMEM((chans, spots), BF16),
            pltpu.VMEM((group, rows * own, total), BF16),
            pltpu.VMEM((group, rows * own, total), BF16),
            pltpu.VMEM((2, 4 * hidden, chans), BF16),
            pltpu.VMEM((chans, chans), BF16),
            pltpu.VMEM((chans, hidden), BF16),
            pltpu.VMEM((2, hidden, total), F32),
            pltpu.VMEM((chans, total), F32),
            pltpu.VMEM((2, 1, spots), F32),
            pltpu.VMEM((rows, total, chans), BF16),
            pltpu.VMEM((chans, spots), BF16),
            pltpu.VMEM((2, chans, spots), BF16),
            pltpu.VMEM((2, chans, spots), BF16),
            pltpu.VMEM((2, chans, spots), F32),
            pltpu.VMEM((2, spots, chans), BF16),
            pltpu.VMEM((2, spots, chans), F32),
            pltpu.VMEM((2, group * (rows * own + PAD), total), F32),
            pltpu.VMEM((group * rows * own, total), F32),
            pltpu.VMEM((own, total, 2 * total), BF16),
            pltpu.VMEM((2, half_rows, total), F32),
            pltpu.VMEM((2 * half_rows, total), F32),
            pltpu.VMEM((2 * half_rows, total), F32),
            pltpu.VMEM((2 * half_rows, total), F32),
            pltpu.VMEM((cols * own, total), F32),
            pltpu.SemaphoreType.DMA((12,)),
            pltpu.SemaphoreType.DMA((12,)),
            pltpu.SemaphoreType.DMA((7,)),
        ],
        compiler_params=pltpu.CompilerParams(
            collective_id=0, has_side_effects=True, vmem_limit_bytes=16777216
        ),
        name="triangles",
    )(*operands)


def panels(rows, mask_rows, mask_all, gain, weight):
    hidden = weight.shape[1] // 4
    mask_float = mask_all.astype(F32)
    normed = (normalize(rows.astype(F32), 2) * gain).astype(BF16)
    proj = jnp.einsum("rnc,ch->hrn", normed, weight, preferred_element_type=F32)
    scale = mask_rows.astype(F32)[:, None] * mask_float[None, :]
    left = (jax.nn.sigmoid(proj[:hidden]) * proj[hidden : 2 * hidden] * scale).astype(BF16)
    right = (jax.nn.sigmoid(proj[2 * hidden : 3 * hidden]) * proj[3 * hidden :] * scale).astype(
        BF16
    )
    return (normed, left, right)


def triangle(rows, mask_rows, mask_all, gain, weight, gate_w, tri_gain, out_w, second):
    normed, left, right = panels(rows, mask_rows, mask_all, gain, weight)
    left = lax.all_to_all(left, "dap", split_axis=0, concat_axis=1, tiled=True)
    right = lax.all_to_all(right, "dap", split_axis=0, concat_axis=1, tiled=True)
    spec = "cki,ckj->cij" if second else "cik,cjk->cij"
    tri = jnp.einsum(spec, left, right, preferred_element_type=F32).astype(BF16)
    tri = lax.all_to_all(tri, "dap", split_axis=1, concat_axis=0, tiled=True)
    gate = jax.nn.sigmoid(jnp.einsum("rnc,cd->rnd", normed, gate_w, preferred_element_type=F32))
    tri_normed = (normalize(tri.astype(F32), 0) * tri_gain[:, None, None]).astype(BF16)
    out = jnp.einsum("hrn,hc->rnc", tri_normed, out_w, preferred_element_type=F32)
    return (rows.astype(F32) + gate * out).astype(BF16)


def by_collectives(pair, residue_mask, *params):
    mask_all = lax.all_gather(residue_mask, "dap", axis=0, tiled=True)
    state = pair
    for layer in range(2):
        gain, weight, gate_w, tri_gain, out_w = (p[layer] for p in params)
        state = triangle(
            state, residue_mask, mask_all, gain, weight, gate_w, tri_gain, out_w, layer == 1
        )
    return state


def solution(mesh):
    devices = mesh.shape["dap"]

    def body(pair, residue_mask, norm_gain, proj_weight, gate_weight, mix_gain, out_weight):
        args = (pair, residue_mask, norm_gain, proj_weight, gate_weight, mix_gain, out_weight)
        group = devices // HALVES
        own = mix_gain.shape[1] // group
        rows, total, chans = pair.shape
        whole = group * HALVES == devices and group & (group - 1) == 0
        whole = whole and own * group == chans == mix_gain.shape[1] == total == 128
        if whole and own == 8 and rows == 4:
            return fused(devices, *args)
        return by_collectives(*args)

    return jax.shard_map(
        body,
        mesh=mesh,
        in_specs=(P("dap", None, None), P("dap"), P(), P(), P(), P(), P()),
        out_specs=P("dap", None, None),
        check_vma=False,
    )
```
